32 devices in a mesh: node: 4 (over y, x), row: 8 (over z, core).
Axes of the slice: x: 2, y: 2, z: 4, core: 2. Of those that a mesh axis runs over, the one named last changes fastest.
Arguments:
- inputs: float32 [16, 32, 128, 128], P(None, 'row'), may hold values from -8 to 8
- diagonal: float32 [32, 128, 128], P('row'), may hold values from 0.05 to 1
- observations: float32 [16, 32, 128, 128], P(None, 'row'), may hold values from -0.0078125 to 0.0078125
- frequencies: float32 [4], replicated, may hold values from 0.2 to 3
- weights: float32 [4], replicated, may hold values from 0.5 to 2
- counts: int32 [4], replicated, may hold values from 3 to 6, as said below
- assignment: int32 [4], replicated, may hold values from 0 to 3, each once
Outputs:
- probe_response: float32 [16, 32, 128, 128], P(None, 'row')
- group_gram: float32 [4, 16, 16], P('node')
The draws below stay inside these ranges and needn't reach their ends.
Inputs may be any that keep to these rules, and one draw needn't show every extreme that they name: `counts`: some node has 6 sweeps and some node 3 in every draw. `assignment`: each node 0 to 3 appears once.
All inputs are finite; a program needn't handle non-finite values.
Results may differ from the reference program's by a relative error of at most 0.0003.
Values sent between devices are 32-bit elements; how exact they have to be, the bound alone decides.
A program may use at most 192 MiB of HBM per device.

```python
import math
import jax
import jax.numpy as jnp
from jax import lax

INPUTS = 16
PROBES = 16
GY = 128
GZ = 128
NODE_DEV = 1
ITERS = 6
QUAD = 4
NX = 32
CELLS = 524288
N_NODE = 4


def draw_inputs(key, part):
    values = jnp.clip(2.0 * jax.random.normal(key, (INPUTS, NX, GY, GZ), jnp.float32), -8.0, 8.0)
    return values.astype(jnp.float32)


def draw_counts(key, part):
    first, second, third = jax.random.split(jax.random.fold_in(key, 17), 3)
    values = jax.random.randint(first, (QUAD,), ITERS // 2, ITERS + 1, jnp.int32)
    top_slot = jax.random.randint(second, (), 0, QUAD, jnp.int32)
    low_slot = (top_slot + 1 + jax.random.randint(third, (), 0, QUAD - 1, jnp.int32)) % QUAD
    values = values.at[top_slot].set(ITERS)
    values = values.at[low_slot].set(ITERS // 2)
    return values.astype(jnp.int32)


def block_scale(stream_key, extent, cuts, least, high):
    gain, own = 1.0, jax.random.fold_in(stream_key, 6)
    for position, blocks in cuts:
        heights = jnp.exp(jax.random.uniform(jax.random.fold_in(own, position), (blocks,), jnp.float32, least / len(cuts), high / len(cuts)))
        gain = gain * jnp.repeat(heights, extent[position] // blocks).reshape([-1 if axis == position else 1 for axis in range(len(extent))])
    return gain


def normal_values(own_key, shape, width, bound, pieces=(), kind=jnp.bfloat16):
    entries = jax.random.normal(own_key, shape, jnp.float32) * width
    if len(pieces) > 0:
        entries = block_scale(own_key, shape, pieces, -0.22, 0.18) * entries
    return jnp.clip(entries, min=-bound, max=bound).astype(kind)


def setup_inputs(seed: int = 0) -> dict:
    seeds = jax.random.split(jax.random.key(seed), 8)
    inputs = draw_inputs(jax.random.fold_in(seeds[7], 71), 0)
    diagonal = jnp.clip(jnp.exp(math.log(1.0) - 2.9957323 * jax.random.uniform(seeds[1], (NX, GY, GZ), jnp.float32) ** block_scale(seeds[1], (NX, GY, GZ), ((0, 8),), -0.2, 0.2)), 0.05, 1.0)
    observations = normal_values(seeds[2], (PROBES, NX, GY, GZ), CELLS ** -0.5, 0.0078125, ((1, 8),), jnp.float32)
    frequencies = jnp.clip(jax.random.uniform(seeds[3], (QUAD,), jnp.float32, 0.2, 3.0), 0.2, 3.0)
    weights = jnp.clip(jnp.exp(jax.random.uniform(seeds[4], (QUAD,), jnp.float32, math.log(0.5), math.log(2.0))), 0.5, 2.0)
    counts = draw_counts(jax.random.fold_in(seeds[7], 71), 0)
    assignment = jax.random.permutation(seeds[6], QUAD).astype(jnp.int32)
    return {"inputs": inputs, "diagonal": diagonal, "observations": observations, "frequencies": frequencies, "weights": weights, "counts": counts, "assignment": assignment}


def relax_step(fields, source, diagonal, shift_val, active):
    padded = jnp.pad(fields, ((0, 0), (0, 0), (1, 1), (1, 1), (1, 1)))
    beside = padded[:, :, 2:, 1:-1, 1:-1] + padded[:, :, :-2, 1:-1, 1:-1]
    beside = beside + padded[:, :, 1:-1, 2:, 1:-1] + padded[:, :, 1:-1, :-2, 1:-1]
    beside = beside + padded[:, :, 1:-1, 1:-1, 2:] + padded[:, :, 1:-1, 1:-1, :-2]
    diag_full = 6.0 + diagonal
    applied = diag_full * fields - beside
    resid_real = source - applied[0] + shift_val * fields[1]
    resid_imag = -applied[1] - shift_val * fields[0]
    denominator = diag_full * diag_full + shift_val * shift_val
    step_real = (diag_full * resid_real + shift_val * resid_imag) / denominator
    step_imag = (diag_full * resid_imag - shift_val * resid_real) / denominator
    return fields + active * jnp.stack([step_real, step_imag], 0)


def reference(inputs, diagonal, observations, frequencies, weights, counts, assignment):
    cells = NX * GY * GZ
    flat_probe = observations.reshape(PROBES, cells)

    def one_node(carry, node_id):
        shift_val = frequencies[node_id]
        fields = jnp.zeros((2,) + inputs.shape, jnp.float32)
        for sweep in range(ITERS):
            active = (sweep < counts[node_id]).astype(jnp.float32)
            fields = relax_step(fields, inputs, diagonal, shift_val, active)
        flat_fields = fields.reshape(2, INPUTS, cells)
        projected = jnp.einsum("aic,pc->aip", flat_fields, flat_probe, precision=lax.Precision.HIGHEST)
        gram_part = jnp.einsum("aic,ajc->ij", flat_fields, flat_fields, precision=lax.Precision.HIGHEST)
        contrib = jnp.einsum("aip,aic->pc", projected, flat_fields, precision=lax.Precision.HIGHEST)
        return carry + weights[node_id] * contrib, weights[node_id] * gram_part

    start = jnp.zeros((PROBES, cells), jnp.float32)
    total, grams = lax.scan(one_node, start, jnp.arange(QUAD, dtype=jnp.int32))
    probe_response = (total / QUAD).reshape(PROBES, NX, GY, GZ)
    group_gram = grams[assignment].reshape(N_NODE, NODE_DEV, INPUTS, INPUTS).sum(1) / cells
    return probe_response, group_gram
```

```python
import functools

import jax
import jax.numpy as jnp
from jax import lax
from jax.experimental import pallas as pl
from jax.experimental.pallas import tpu as pltpu
from jax.sharding import PartitionSpec as P

NODE_DEV = 1
ITERS = 6
VMEM_LIMIT = 62 * 1024 * 1024
STEP = 8
PAIR = 2
START = 6
CHUNK = 16
MESH = pl.DeviceIdType.MESH


def sweep_kernel(halo, own, planes, counts_ref, freq_ref, obs_ref, *refs):
    pieces = refs[:-13]
    fhl_ref, proj_ref, gram_ref, acc_ref, src_ref, xa_ref, xb_ref, f_ref, st_ref, gr_ref, gi_ref, sems, obs_sem = refs[-13:]
    total = planes + 2 * halo
    win = own + 2 * halo
    cols, gz = src_ref.shape[2:]
    quad = counts_ref.shape[0]
    copies = []
    at = 0
    for n, piece in enumerate(pieces):
        copies.append(
            pltpu.make_async_copy(piece, src_ref.at[pl.ds(at, piece.shape[0])], sems.at[n])
        )
        at += piece.shape[0]
    for copy in copies:
        copy.start()
    for copy in copies:
        copy.wait()

    lane = lax.broadcasted_iota(jnp.int32, (cols, gz), 1)
    first = lane == 0
    last = lane == gz - 1

    def beside(v):
        return jnp.where(first, 0.0, pltpu.roll(v, 1, 1)) + jnp.where(
            last, 0.0, pltpu.roll(v, gz - 1, 1)
        )

    def gain(p, y):
        return (
            jnp.broadcast_to(gr_ref[p, pl.ds(y, 1), :], (cols, gz)),
            jnp.broadcast_to(gi_ref[p, pl.ds(y, 1), :], (cols, gz)),
        )

    def stage(x_ref, p, y):
        for q in range(PAIR):
            for comp in range(2):
                rows = [x_ref[comp, p + q, y - 1 + t] for t in range(STEP + 2)]
                for t in range(STEP):
                    n = (rows[t] + rows[t + 2]) + beside(rows[t + 1])
                    if comp == 0:
                        n = n + src_ref[p + q, y + t]
                    st_ref[comp, q, t] = n

    def combine(x_ref, p, y, put):
        for q in range(PAIR):
            for t in range(STEP):
                nu = st_ref[0, q, t] + (x_ref[0, p + q - 1, y + t] + x_ref[0, p + q + 1, y + t])
                nw = st_ref[1, q, t] + (x_ref[1, p + q - 1, y + t] + x_ref[1, p + q + 1, y + t])
                gr, gi = gain(p + q, y + t)
                put(p + q, y + t, gr * nu - gi * nw, gr * nw + gi * nu)

    def sweep(x_ref, radius, put):
        low = halo - radius
        groups = (own + 2 * radius + STEP - 1) // STEP
        end = low + STEP * groups
        pairs = (planes + 2 * radius) // PAIR
        stage(x_ref, low, low)

        def body(j, c):
            p, y = c
            wrap = y + STEP >= end
            ny = jnp.where(wrap, low, y + STEP)
            np_ = jnp.minimum(jnp.where(wrap, p + PAIR, p), low + planes + 2 * radius - PAIR)
            combine(x_ref, p, y, put)
            stage(x_ref, np_, ny)
            return np_, ny

        lax.fori_loop(0, groups * pairs, body, (low, low))

    def node(k, c):
        w = freq_ref[k]
        count = counts_ref[k]
        low1 = halo + 1 - count

        def gains(p, c):
            part = src_ref[p, win:, :, :].reshape(gr_ref.shape[1:])
            d = 6.0 + part
            inv = jnp.where(part > 0.0, 1.0 / (d * d + w * w), 0.0)
            gr_ref[p] = d * inv
            gi_ref[p] = -w * inv
            return c

        lax.fori_loop(low1, total - low1, gains, 0)

        groups1 = (own + 2 * (count - 1) + START - 1) // START

        def start_plane(p, c):
            def rows(j, c):
                y = low1 + START * j
                for t in range(START):
                    b = src_ref[p, y + t]
                    gr, gi = gain(p, y + t)
                    xa_ref[0, p, y + t] = gr * b
                    xa_ref[1, p, y + t] = gi * b
                return c

            return lax.fori_loop(0, groups1, rows, c)

        lax.fori_loop(low1, low1 + planes + 2 * (count - 1), start_plane, 0)

        def into(ref):
            def put(p, y, u, v):
                ref[0, p, y] = u
                ref[1, p, y] = v

            return put

        def put_last(p, y, u, v):
            row = (p - halo) * own + (y - halo)
            f_ref[row, k, 0] = u
            f_ref[row, k, 1] = v

        inner = count - 2

        def pair(i, c):
            s = 2 * i + 2
            sweep(xa_ref, count - s, into(xb_ref))

            @pl.when(2 * i + 1 < inner)
            def _():
                sweep(xb_ref, count - s - 1, into(xa_ref))

            return c

        lax.fori_loop(0, (inner + 1) // 2, pair, 0)

        @pl.when(inner % 2 == 1)
        def _():
            sweep(xb_ref, 0, put_last)

        @pl.when(inner % 2 == 0)
        def _():
            sweep(xa_ref, 0, put_last)

        return c

    lax.fori_loop(0, quad, node, 0)

    nf = quad * 2 * cols
    acc_ref[...] = jnp.zeros_like(acc_ref)

    def products(j, c):
        his, los, ohis, olos = [], [], [], []
        for t in range(2):
            f = f_ref[2 * j + t].reshape(nf, gz)
            hi = f.astype(jnp.bfloat16)
            lo = (f - hi.astype(jnp.float32)).astype(jnp.bfloat16)
            o = obs_ref[2 * j + t]
            ohi = o.astype(jnp.bfloat16)
            olo = (o - ohi.astype(jnp.float32)).astype(jnp.bfloat16)
            fhl_ref[2 * j + t, :nf] = hi
            fhl_ref[2 * j + t, nf:] = lo
            his.append(hi)
            los.append(lo)
            ohis.append(ohi)
            olos.append(olo)
        hi = jnp.concatenate(his, 1)
        left = jnp.concatenate([hi, jnp.concatenate(ohis, 1), jnp.concatenate(olos, 1)], 0)
        right = jnp.concatenate([hi, jnp.concatenate(los, 1)], 0)
        acc_ref[...] += lax.dot_general(
            left, right, (((1,), (1,)), ((), ())), preferred_element_type=jnp.float32
        )
        return c

    lax.fori_loop(0, f_ref.shape[0] // 2, products, 0)

    probes = obs_ref.shape[1]
    proj_ref[...] = (
        acc_ref[nf : nf + probes, :nf] + acc_ref[nf + probes :, :nf] + acc_ref[nf : nf + probes, nf:]
    )
    cross = acc_ref[:nf, nf:]
    gram = acc_ref[:nf, :nf] + cross + cross.T
    block = lax.broadcasted_iota(jnp.int32, (cols, nf), 1) // cols
    diag = jnp.zeros((cols, nf), jnp.float32)
    for n in range(nf // cols):
        diag = diag + jnp.where(block == n, gram[n * cols : (n + 1) * cols], 0.0)
    gram_ref[...] = diag


def tail_kernel(parts, count, planes, own, cells, weights_ref, assign_ref, proj_ref, part_ref, fhl_hbm,
                out_ref, gram_ref, f_ref, prow_ref, psum_ref, pnode_ref, grow_ref, gsum_ref, gnode_ref,
                f_sem, psend, precv, pnsend, pnrecv, gsend, grecv, gnsend, gnrecv, osend, orecv):
    me = lax.axis_index("node")
    row = lax.axis_index("row")
    probes, nf = proj_ref.shape
    cols = part_ref.shape[0]
    quad = weights_ref.shape[0]
    gz = out_ref.shape[1]
    gy = own * parts
    out = out_ref.reshape(probes, planes, gy, gz)

    barrier = pltpu.get_barrier_semaphore()
    for d in range(1, count):
        pl.semaphore_signal(barrier, inc=1, device_id={"row": lax.rem(row + d, count)}, device_id_type=MESH)
    for d in range(1, parts):
        pl.semaphore_signal(barrier, inc=1, device_id={"node": lax.rem(me + d, parts)}, device_id_type=MESH)
    load = pltpu.make_async_copy(fhl_hbm, f_ref, f_sem)
    load.start()
    pl.semaphore_wait(barrier, count - 1 + parts - 1)

    def exchange(axis, size, index, src, buf, send, recv):
        copies = []
        for d in range(1, size):
            copies.append(
                pltpu.make_async_remote_copy(
                    src_ref=src,
                    dst_ref=buf.at[index],
                    send_sem=send.at[d - 1],
                    recv_sem=recv.at[d - 1],
                    device_id={axis: lax.rem(index + d, size)},
                    device_id_type=MESH,
                )
            )
            copies[-1].start()
        return copies

    def collect(size, index, src, buf, copies):
        buf[index] = src[...]
        for copy in copies:
            copy.wait()
        total = buf[0]
        for n in range(1, size):
            total = total + buf[n]
        return total

    pcopies = exchange("row", count, row, proj_ref, prow_ref, psend, precv)
    gcopies = exchange("row", count, row, part_ref, grow_ref, gsend, grecv)
    psum_ref[...] = collect(count, row, proj_ref, prow_ref, pcopies)
    pncopies = exchange("node", parts, me, psum_ref, pnode_ref, pnsend, pnrecv)
    proj = collect(parts, me, psum_ref, pnode_ref, pncopies)

    lane = lax.broadcasted_iota(jnp.int32, (1, nf), 1) // (2 * cols)
    scale = jnp.zeros((1, nf), jnp.float32)
    for k in range(quad):
        scale = jnp.where(lane == k, weights_ref[k] / quad, scale)
    hi, lo = split(proj * scale)
    pw = jnp.concatenate(
        [jnp.concatenate([hi, hi], 1), jnp.concatenate([lo, jnp.zeros_like(lo)], 1)], 0
    )
    load.wait()

    size = min(CHUNK, own)
    per = own // size
    chunks = planes * per

    def respond(ch):
        plane, y0 = ch // per, (ch % per) * size

        def pair(j, c):
            r = plane * own + y0 + 2 * j
            right = jnp.concatenate([f_ref[r], f_ref[r + 1]], 1)
            both = jnp.dot(pw, right, preferred_element_type=jnp.float32)
            both = both[:probes] + both[probes:]
            at = plane * gy + me * own + y0 + 2 * j
            out_ref[pl.ds(at, probes, stride=planes * gy), :] = both[:, :gz]
            out_ref[pl.ds(at + 1, probes, stride=planes * gy), :] = both[:, gz:]
            return c

        lax.fori_loop(0, size // 2, pair, 0)

    def send(ch, owner, target, slot):
        plane, y0 = ch // per, (ch % per) * size
        view = out.at[:, plane, pl.ds(pl.multiple_of(owner * own + y0, 8), size), :]
        return pltpu.make_async_remote_copy(
            src_ref=view,
            dst_ref=view,
            send_sem=osend.at[slot, ch],
            recv_sem=orecv.at[slot, ch],
            device_id={"node": target},
            device_id_type=MESH,
        )

    started = []
    if parts == 4:
        near = me + 1 - 2 * lax.rem(me, 2)
        far = lax.rem(me + 2, 4)

        def launch(ch):
            for slot, target in ((0, near), (1, far)):
                copy = send(ch, me, target, slot)
                copy.start()
                started.append(copy)

        respond(0)
        for ch in range(1, chunks):
            respond(ch)
            launch(ch - 1)
        launch(chunks - 1)
        for ch in range(chunks):
            a, b = send(ch, near, near, 0), send(ch, far, far, 1)
            a.wait_recv()
            b.wait_recv()
            copy = send(ch, near, far, 2) if ch % 2 else send(ch, far, near, 2)
            copy.start()
            started.append(copy)
    else:
        for ch in range(chunks):
            respond(ch)
            for d in range(1, parts):
                copy = send(ch, me, lax.rem(me + d, parts), d - 1)
                copy.start()
                started.append(copy)

    gsum_ref[...] = collect(count, row, part_ref, grow_ref, gcopies)
    gncopies = exchange("node", parts, me, gsum_ref, gnode_ref, gnsend, gnrecv)
    diag = collect(parts, me, gsum_ref, gnode_ref, gncopies)
    source = lax.broadcasted_iota(jnp.int32, (nf, cols), 0)
    column = lax.broadcasted_iota(jnp.int32, (nf, cols), 1)
    total = jnp.zeros((cols, cols), jnp.float32)
    for m in range(NODE_DEV):
        node = assign_ref[me * NODE_DEV + m]
        pick = ((source // (2 * cols) == node) & (source % cols == column)).astype(jnp.bfloat16)
        rest = diag
        picked = jnp.zeros((cols, cols), jnp.float32)
        for _ in range(3):
            piece = rest.astype(jnp.bfloat16)
            rest = rest - piece.astype(jnp.float32)
            picked = picked + jnp.dot(piece, pick, preferred_element_type=jnp.float32)
        total = total + weights_ref[node] * picked
    gram_ref[...] = total / cells

    if parts == 4:
        for ch in range(chunks):
            diagonal = lax.rem(near + 2, 4)
            send(ch, diagonal, near, 2).wait_recv()
        for copy in started:
            copy.wait_send()
    else:
        for ch in range(chunks):
            for d in range(1, parts):
                send(ch, lax.rem(me + parts - d, parts), me, d - 1).wait_recv()
        for copy in started:
            copy.wait_send()


def split(v):
    hi = v.astype(jnp.bfloat16)
    return hi, (v - hi.astype(jnp.float32)).astype(jnp.bfloat16)


def local(inputs, diagonal, observations, frequencies, weights, counts, assignment):
    parts = lax.axis_size("node")
    part = lax.axis_index("node")
    cols, planes, gy, gz = inputs.shape
    probes = observations.shape[0]
    quad = frequencies.shape[0]
    own = gy // parts
    halo = ITERS - 1
    win = own + 2 * halo
    extra = -(-(win + 4) // cols)
    nf = quad * 2 * cols
    local_rows = planes * own

    window = jnp.pad(inputs, ((0, 0), (0, 0), (halo, halo), (0, 0)))
    window = lax.dynamic_slice_in_dim(window, part * own, win, 2).transpose(1, 2, 0, 3)
    diag = jnp.pad(diagonal, ((0, 0), (halo, halo), (0, 0)))
    diag = lax.dynamic_slice_in_dim(diag, part * own, win, 1)
    diag = jnp.pad(diag, ((0, 0), (0, extra * cols - win), (0, 0)))
    packed = jnp.concatenate([window, diag.reshape(planes, extra, cols, gz)], 1)

    count = lax.axis_size("row")
    lows, highs = [], []
    for hop in range(1, -(-halo // planes) + 1):
        size = min(planes, halo - (hop - 1) * planes)
        up = [(i, i + hop) for i in range(count - hop)]
        down = [(j, i) for i, j in up]
        lows.insert(0, lax.ppermute(packed[planes - size :], "row", up))
        highs.append(lax.ppermute(packed[:size], "row", down))
    pieces = lows + [packed] + highs

    obs = lax.dynamic_slice_in_dim(observations, part * own, own, 2)
    obs = obs.transpose(1, 2, 0, 3).reshape(local_rows, probes, gz)

    total = planes + 2 * halo
    vmem = pl.BlockSpec(memory_space=pltpu.VMEM)
    smem = pl.BlockSpec(memory_space=pltpu.SMEM)
    fhl, proj, diags = pl.pallas_call(
        functools.partial(sweep_kernel, halo, own, planes),
        out_shape=(
            jax.ShapeDtypeStruct((local_rows, 2 * nf, gz), jnp.bfloat16),
            jax.ShapeDtypeStruct((probes, nf), jnp.float32),
            jax.ShapeDtypeStruct((cols, nf), jnp.float32),
        ),
        in_specs=[smem, smem, vmem] + [pl.BlockSpec(memory_space=pl.ANY)] * len(pieces),
        out_specs=(vmem, vmem, vmem),
        scratch_shapes=[
            pltpu.VMEM((nf + 2 * probes, 2 * nf), jnp.float32),
            pltpu.VMEM((total, win + extra, cols, gz), jnp.float32),
            pltpu.VMEM((2, total, win + 4, cols, gz), jnp.float32),
            pltpu.VMEM((2, total, win + 4, cols, gz), jnp.float32),
            pltpu.VMEM((local_rows, quad, 2, cols, gz), jnp.float32),
            pltpu.VMEM((2, PAIR, STEP, cols, gz), jnp.float32),
            pltpu.VMEM((total, extra * cols, gz), jnp.float32),
            pltpu.VMEM((total, extra * cols, gz), jnp.float32),
            pltpu.SemaphoreType.DMA((len(pieces),)),
            pltpu.SemaphoreType.DMA,
        ],
        compiler_params=pltpu.CompilerParams(vmem_limit_bytes=VMEM_LIMIT),
        name="sweeps",
    )(counts, frequencies, obs, *pieces)

    cells = planes * gy * gz * count
    chunks = planes * (own // min(CHUNK, own))
    dma = pltpu.SemaphoreType.DMA
    response, group_gram = pl.pallas_call(
        functools.partial(tail_kernel, parts, count, planes, own, cells),
        out_shape=(
            jax.ShapeDtypeStruct((probes * planes * gy, gz), jnp.float32),
            jax.ShapeDtypeStruct((cols, cols), jnp.float32),
        ),
        in_specs=[smem, smem, vmem, vmem, pl.BlockSpec(memory_space=pl.ANY)],
        out_specs=(vmem, vmem),
        scratch_shapes=[
            pltpu.VMEM((local_rows, 2 * nf, gz), jnp.bfloat16),
            pltpu.VMEM((count, probes, nf), jnp.float32),
            pltpu.VMEM((probes, nf), jnp.float32),
            pltpu.VMEM((parts, probes, nf), jnp.float32),
            pltpu.VMEM((count, cols, nf), jnp.float32),
            pltpu.VMEM((cols, nf), jnp.float32),
            pltpu.VMEM((parts, cols, nf), jnp.float32),
            dma,
            dma((count - 1,)),
            dma((count - 1,)),
            dma((parts - 1,)),
            dma((parts - 1,)),
            dma((count - 1,)),
            dma((count - 1,)),
            dma((parts - 1,)),
            dma((parts - 1,)),
            dma((parts - 1, chunks)),
            dma((parts - 1, chunks)),
        ],
        compiler_params=pltpu.CompilerParams(
            vmem_limit_bytes=VMEM_LIMIT, collective_id=0, has_side_effects=True
        ),
        name="tail",
    )(weights, assignment, proj, diags, fhl)
    return response.reshape(probes, planes, gy, gz), group_gram[None]


def solution(mesh):
    placed = (
        P(None, "row", None, None),
        P("row", None, None),
        P(None, "row", None, None),
        P(),
        P(),
        P(),
        P(),
    )
    return jax.shard_map(
        local,
        mesh=mesh,
        in_specs=placed,
        out_specs=(P(None, "row", None, None), P("node", None, None)),
        check_vma=False,
    )
```

```python
import functools

import jax
import jax.numpy as jnp
from jax import lax
from jax.experimental import pallas as pl
from jax.experimental.pallas import tpu as pltpu
from jax.sharding import PartitionSpec as P

NODE_DEV = 1
ITERS = 6
EXCHANGE_VMEM = 8 * 1024 * 1024
SWEEP_VMEM = 30 * 1024 * 1024
TAIL_VMEM = 16 * 1024 * 1024
STEP = 8
OFF = 1
EDGE = 8
GROUPS = 2
MERGE = 2
START = 6
CHUNK = 16
MESH = pl.DeviceIdType.MESH


def exchange_kernel(halo, own, parts, count, inputs, diagonal, observations, src_ref, dg_ref, ob_ref,
                    nat_ref, onat_ref, load_sem, dload_sem, oload_sem, send_sem, recv_sem, dsend_sem, drecv_sem):
    me = lax.axis_index("node")
    row = lax.axis_index("row")
    cols, planes, gy, gz = inputs.shape
    probes = observations.shape[0]
    size = nat_ref.shape[2]
    start = pl.multiple_of(jnp.clip(me * own - EDGE, 0, gy - size), 8)
    top = halo + planes
    last = top + halo - 1

    loads = []
    for j in range(planes):
        loads.append(
            pltpu.make_async_copy(inputs.at[:, j, pl.ds(start, size), :], nat_ref.at[halo + j], load_sem.at[j])
        )
        loads[-1].start()
    dload = pltpu.make_async_copy(
        diagonal.at[:, pl.ds(start, size), :], dg_ref.at[pl.ds(halo, planes)], dload_sem
    )
    dload.start()
    oloads = []
    for j in range(planes):
        rows = pl.ds(pl.multiple_of(me * own, 8), own)
        oloads.append(
            pltpu.make_async_copy(observations.at[:, j, rows, :], onat_ref.at[j], oload_sem.at[j])
        )
        oloads[-1].start()

    barrier = pltpu.get_barrier_semaphore()
    for hop in (-2, -1, 1, 2):
        @pl.when((row + hop >= 0) & (row + hop < count))
        def _():
            pl.semaphore_signal(barrier, inc=1, device_id={"row": row + hop}, device_id_type=MESH)
    pl.semaphore_wait(barrier, jnp.minimum(row, 2) + jnp.minimum(count - 1 - row, 2))

    def plane(source, target, send, to):
        return pltpu.make_async_remote_copy(
            src_ref=nat_ref.at[source],
            dst_ref=nat_ref.at[target],
            send_sem=send_sem.at[send],
            recv_sem=recv_sem.at[target],
            device_id={"row": to},
            device_id_type=MESH,
        )

    def strip(source, target, size, slot, to):
        return pltpu.make_async_remote_copy(
            src_ref=dg_ref.at[pl.ds(source, size)],
            dst_ref=dg_ref.at[pl.ds(target, size)],
            send_sem=dsend_sem.at[slot],
            recv_sem=drecv_sem.at[slot],
            device_id={"row": to},
            device_id_type=MESH,
        )

    even = lax.rem(row, 2) == 0
    far = halo - planes
    up = [plane(halo + j, far + j, far + j, row + 1) for j in range(planes)]
    up_far = plane(top - 1, 0, 0, row + 2)
    up_pass = plane(halo - 1, 0, last + 1, row + 1)
    down = [plane(halo + j, top + j, top + j, row - 1) for j in range(planes)]
    down_far = plane(halo, last, last, row - 2)
    down_pass = plane(top, last, last + 2, row - 1)
    strips = (
        (row + 1 < count, row >= 1, strip(halo, far, planes, 0, row + 1)),
        (row + 2 < count, row >= 2, strip(top - far, 0, far, 1, row + 2)),
        (row >= 1, row + 1 < count, strip(halo, top, planes, 2, row - 1)),
        (row >= 2, row + 2 < count, strip(halo, top + planes, far, 3, row - 2)),
    )
    has_up, has_down = row + 1 < count, row >= 1
    direct_up, direct_down = even & (row + 2 < count), ~even & (row >= 2)
    pass_up, pass_down = even & has_down & has_up, ~even & has_up & has_down

    def when(flag, *actions):
        @pl.when(flag)
        def _():
            for action in actions:
                action()

    for copy in loads:
        copy.wait()
    dload.wait()
    when(has_up, up[-1].start)
    when(has_down, down[0].start)
    when(direct_up, up_far.start)
    when(direct_down, down_far.start)
    for sends, _, copy in strips:
        when(sends, copy.start)
    for j in range(1, planes):
        when(has_up, up[planes - 1 - j].start)
        when(has_down, down[j].start)

    base = start - (me * own - 2 * EDGE)

    def turn(p):
        def block(o, c):
            at = pl.multiple_of(8 * o, 8)
            for h in range(cols // 8):
                value = nat_ref[p, 8 * h : 8 * h + 8, pl.ds(at, 8), :]
                src_ref[p, pl.ds(base + at, 8), 8 * h : 8 * h + 8, :] = jnp.swapaxes(value, 0, 1)
            return c

        lax.fori_loop(0, size // 8, block, 0)

    for j in range(planes):
        turn(halo + j)

    for copy in oloads:
        copy.wait()

    def probe(n, c):
        p, at = n // (own // 8), pl.multiple_of(lax.rem(n, own // 8) * 8, 8)
        for h in range(probes // 8):
            value = jnp.swapaxes(onat_ref[p, 8 * h : 8 * h + 8, pl.ds(at, 8), :], 0, 1)
            ob_ref[pl.ds(8 * n, 8), 8 * h : 8 * h + 8, :] = value
        return c

    lax.fori_loop(0, planes * (own // 8), probe, 0)

    when(has_down, up[-1].wait_recv)
    when(pass_up, up_pass.start)
    when(has_up, down[0].wait_recv)
    when(pass_down, down_pass.start)
    when(has_down, lambda: turn(halo - 1))
    when(has_up, lambda: turn(top))
    for j in range(1, planes):
        low, high = planes - 1 - j, j
        when(has_down, up[low].wait_recv, lambda: turn(far + low))
        when(has_up, down[high].wait_recv, lambda: turn(top + high))
    when(row >= 2, up_far.wait_recv, lambda: turn(0))
    when(row + 2 < count, down_far.wait_recv, lambda: turn(last))
    for _, receives, copy in strips:
        when(receives, copy.wait_recv)

    def clear(at, n):
        def one(p, c):
            src_ref[p] = jnp.zeros(src_ref.shape[1:], jnp.float32)
            dg_ref[p] = jnp.zeros(dg_ref.shape[1:], jnp.float32)
            return c

        return lambda: lax.fori_loop(at, at + n, one, 0)

    when(row < 1, clear(far, planes))
    when(row < 2, clear(0, far))
    when(row + 1 >= count, clear(top, planes))
    when(row + 2 >= count, clear(top + planes, far))

    def edge(at):
        def one(p, c):
            src_ref[p, at : at + EDGE] = jnp.zeros((EDGE,) + src_ref.shape[2:], jnp.float32)
            return c

        return lambda: lax.fori_loop(0, top + halo, one, 0)

    when(me == 0, edge(EDGE))
    when(me == parts - 1, edge(own + 2 * EDGE))

    when(has_up, *[copy.wait_send for copy in up])
    when(has_down, *[copy.wait_send for copy in down])
    when(direct_up, up_far.wait_send)
    when(direct_down, down_far.wait_send)
    when(pass_up, up_pass.wait_send)
    when(pass_down, down_pass.wait_send)
    for sends, _, copy in strips:
        when(sends, copy.wait_send)


def sweep_kernel(halo, own, planes, counts_ref, freq_ref, obs_ref, src_ref, dg_ref, fhl_ref, proj_ref, gram_ref,
                 acc_ref, xa_ref, xb_ref, near_ref, st_ref, gr_ref, gi_ref):
    total = planes + 2 * halo
    cols, gz = src_ref.shape[2:]
    quad = counts_ref.shape[0]
    size = dg_ref.shape[1]
    me = lax.axis_index("node")
    start = jnp.clip(me * own - EDGE, 0, own * lax.axis_size("node") - size)
    lift = me * own - halo - OFF - start + EDGE
    skew = 2 * EDGE - halo - OFF

    gap = lax.broadcasted_iota(jnp.int32, (2 * gz, gz), 0) % gz - lax.broadcasted_iota(
        jnp.int32, (2 * gz, gz), 1
    )
    near_ref[...] = ((gap == 1) | (gap == -1)).astype(jnp.bfloat16)
    lane = lax.broadcasted_iota(jnp.int32, (cols, gz), 1)
    first = lane == 0
    last = lane == gz - 1

    def beside(v):
        return jnp.where(first, 0.0, pltpu.roll(v, 1, 1)) + jnp.where(
            last, 0.0, pltpu.roll(v, gz - 1, 1)
        )

    def gain(p, y):
        return (
            jnp.broadcast_to(gr_ref[p, pl.ds(y + lift, 1), :], (cols, gz)),
            jnp.broadcast_to(gi_ref[p, pl.ds(y + lift, 1), :], (cols, gz)),
        )

    def stage(x_ref, spots, parity):
        for g, (p, y) in enumerate(spots):
            us = [[x_ref[0, p + q, y - 1 + t] for t in range(STEP + 2)] for q in range(2)]
            for t in range(STEP):
                for q in range(2):
                    n = (us[q][t] + us[q][t + 2]) + (us[1 - q][t + 1] + src_ref[p + q, y + skew + t])
                    st_ref[g, 0, q, parity + t] = n + beside(us[q][t + 1])
        for g, (p, y) in enumerate(spots):
            ws = [[x_ref[1, p + q, y - 1 + t] for t in range(STEP + 2)] for q in range(2)]
            left = []
            for t in range(STEP):
                for q in range(2):
                    hi, lo = split(ws[q][t + 1])
                    left.append(jnp.concatenate([hi, lo], 1))
            z = jnp.dot(jnp.concatenate(left, 0), near_ref[...], preferred_element_type=jnp.float32)
            for t in range(STEP):
                for q in range(2):
                    n = (ws[q][t] + ws[q][t + 2]) + ws[1 - q][t + 1]
                    at = (2 * t + q) * cols
                    st_ref[g, 1, q, parity + t] = n + z[at : at + cols]

    def combine(x_ref, spots, put, parity):
        for g, (p, y) in enumerate(spots):
            for t in range(STEP):
                for q in range(2):
                    side = p + 3 * q - 1
                    nu = st_ref[g, 0, q, parity + t] + x_ref[0, side, y + t]
                    nw = st_ref[g, 1, q, parity + t] + x_ref[1, side, y + t]
                    gr, gi = gain(p + q, y + t)
                    put(p + q, y + t, gr * nu - gi * nw, gr * nw + gi * nu)

    def sweep(x_ref, radius, put):
        first_plane = halo - radius
        low = first_plane + OFF
        parity = lax.rem(low, 2)
        groups = (own + 2 * radius + STEP - 1) // STEP
        end = low + STEP * groups
        top = first_plane + planes + 2 * radius - 2
        pairs = (planes + 2 * radius) // 2

        def after(p, y):
            wrap = y + STEP >= end
            past = p + 2 > top
            ny = jnp.where(wrap, jnp.where(past, y, low), y + STEP)
            return jnp.where(wrap & ~past, p + 2, p), ny

        spots = [(first_plane, low)]
        for _ in range(GROUPS - 1):
            spots.append(after(*spots[-1]))
        stage(x_ref, spots, parity)

        def body(j, spots):
            nxt = [after(*spots[-1])]
            for _ in range(GROUPS - 1):
                nxt.append(after(*nxt[-1]))
            combine(x_ref, spots, put, parity)
            stage(x_ref, nxt, parity)
            return tuple(nxt)

        lax.fori_loop(0, (groups * pairs + GROUPS - 1) // GROUPS, body, tuple(spots))

    def node(k, c):
        w = freq_ref[k]
        count = counts_ref[k]
        low1 = halo + 1 - count

        def gains(p, c):
            part = dg_ref[p]
            d = 6.0 + part
            inv = jnp.where(part > 0.0, 1.0 / (d * d + w * w), 0.0)
            rows = slice(EDGE, EDGE + size)
            for ref, value in ((gr_ref, d * inv), (gi_ref, -w * inv)):
                ref[p, :EDGE] = jnp.zeros((EDGE, gz), jnp.float32)
                ref[p, rows] = value
                ref[p, EDGE + size :] = jnp.zeros((EDGE, gz), jnp.float32)
            return c

        lax.fori_loop(low1, total - low1, gains, 0)

        groups1 = (own + 2 * (count - 1) + START - 1) // START

        def start_plane(p, c):
            def rows(j, c):
                y = low1 + OFF + START * j
                for t in range(START):
                    b = src_ref[p, y + skew + t]
                    gr, gi = gain(p, y + t)
                    xa_ref[0, p, y + t] = gr * b
                    xa_ref[1, p, y + t] = gi * b
                return c

            return lax.fori_loop(0, groups1, rows, c)

        lax.fori_loop(low1, low1 + planes + 2 * (count - 1), start_plane, 0)

        def into(ref):
            def put(p, y, u, v):
                ref[0, p, y] = u
                ref[1, p, y] = v

            return put

        def put_last(p, y, u, v):
            row = (p - halo) * own + (y - halo - OFF)
            for comp, value in ((0, u), (1, v)):
                hi, lo = split(value)
                fhl_ref[row, 0, k, comp] = hi
                fhl_ref[row, 1, k, comp] = lo

        inner = count - 2

        def pair(i, c):
            s = 2 * i + 2
            sweep(xa_ref, count - s, into(xb_ref))

            @pl.when(2 * i + 1 < inner)
            def _():
                sweep(xb_ref, count - s - 1, into(xa_ref))

            return c

        lax.fori_loop(0, (inner + 1) // 2, pair, 0)

        @pl.when(inner % 2 == 1)
        def _():
            sweep(xb_ref, 0, put_last)

        @pl.when(inner % 2 == 0)
        def _():
            sweep(xa_ref, 0, put_last)

        return c

    lax.fori_loop(0, quad, node, 0)

    nf = quad * 2 * cols
    acc_ref[...] = jnp.zeros_like(acc_ref)

    def products(j, c):
        total = None
        for m in range(MERGE):
            his, los, ohis, olos = [], [], [], []
            for t in range(2):
                row = 2 * (MERGE * j + m) + t
                his.append(fhl_ref[row, 0].reshape(nf, gz))
                los.append(fhl_ref[row, 1].reshape(nf, gz))
                ohi, olo = split(obs_ref[row])
                ohis.append(ohi)
                olos.append(olo)
            hi = jnp.concatenate(his, 1)
            left = jnp.concatenate([hi, jnp.concatenate(ohis, 1), jnp.concatenate(olos, 1)], 0)
            right = jnp.concatenate([hi, jnp.concatenate(los, 1)], 0)
            part = lax.dot_general(
                left, right, (((1,), (1,)), ((), ())), preferred_element_type=jnp.float32
            )
            total = part if total is None else total + part
        acc_ref[...] += total
        return c

    lax.fori_loop(0, fhl_ref.shape[0] // (2 * MERGE), products, 0)

    probes = obs_ref.shape[1]
    proj_ref[...] = (
        acc_ref[nf : nf + probes, :nf] + acc_ref[nf + probes :, :nf] + acc_ref[nf : nf + probes, nf:]
    )
    cross = acc_ref[:nf, nf:]
    gram = acc_ref[:nf, :nf] + cross + cross.T
    block = lax.broadcasted_iota(jnp.int32, (cols, nf), 1) // cols
    diag = jnp.zeros((cols, nf), jnp.float32)
    for n in range(nf // cols):
        diag = diag + jnp.where(block == n, gram[n * cols : (n + 1) * cols], 0.0)
    gram_ref[...] = diag


def tail_kernel(parts, count, planes, own, cells, weights_ref, assign_ref, proj_ref, part_ref, f_ref,
                out_ref, gram_ref, prow_ref, psum_ref, pnode_ref, grow_ref, gsum_ref, gnode_ref,
                psend, precv, pnsend, pnrecv, gsend, grecv, gnsend, gnrecv, osend, orecv):
    me = lax.axis_index("node")
    row = lax.axis_index("row")
    probes, nf = proj_ref.shape
    cols = part_ref.shape[0]
    quad = weights_ref.shape[0]
    gz = out_ref.shape[1]
    gy = own * parts
    out = out_ref.reshape(probes, planes, gy, gz)

    barrier = pltpu.get_barrier_semaphore()
    for d in range(1, count):
        pl.semaphore_signal(barrier, inc=1, device_id={"row": lax.rem(row + d, count)}, device_id_type=MESH)
    for d in range(1, parts):
        pl.semaphore_signal(barrier, inc=1, device_id={"node": lax.rem(me + d, parts)}, device_id_type=MESH)
    pl.semaphore_wait(barrier, count - 1 + parts - 1)

    def exchange(axis, size, index, src, buf, send, recv):
        copies = []
        for d in range(1, size):
            copies.append(
                pltpu.make_async_remote_copy(
                    src_ref=src,
                    dst_ref=buf.at[index],
                    send_sem=send.at[d - 1],
                    recv_sem=recv.at[d - 1],
                    device_id={axis: lax.rem(index + d, size)},
                    device_id_type=MESH,
                )
            )
            copies[-1].start()
        return copies

    def collect(size, index, src, buf, copies):
        buf[index] = src[...]
        for copy in copies:
            copy.wait()
        total = buf[0]
        for n in range(1, size):
            total = total + buf[n]
        return total

    pcopies = exchange("row", count, row, proj_ref, prow_ref, psend, precv)
    gcopies = exchange("row", count, row, part_ref, grow_ref, gsend, grecv)
    psum_ref[...] = collect(count, row, proj_ref, prow_ref, pcopies)
    pncopies = exchange("node", parts, me, psum_ref, pnode_ref, pnsend, pnrecv)
    proj = collect(parts, me, psum_ref, pnode_ref, pncopies)

    lane = lax.broadcasted_iota(jnp.int32, (1, nf), 1) // (2 * cols)
    scale = jnp.zeros((1, nf), jnp.float32)
    for k in range(quad):
        scale = jnp.where(lane == k, weights_ref[k] / quad, scale)
    hi, lo = split(proj * scale)
    pw = jnp.concatenate(
        [jnp.concatenate([hi, hi], 1), jnp.concatenate([lo, jnp.zeros_like(lo)], 1)], 0
    )

    size = min(CHUNK, own)
    per = own // size
    chunks = planes * per

    def respond(ch):
        plane, y0 = ch // per, (ch % per) * size

        def pair(j, c):
            r = plane * own + y0 + 2 * j
            right = jnp.concatenate([f_ref[r], f_ref[r + 1]], 1)
            both = jnp.dot(pw, right, preferred_element_type=jnp.float32)
            both = both[:probes] + both[probes:]
            at = plane * gy + me * own + y0 + 2 * j
            out_ref[pl.ds(at, probes, stride=planes * gy), :] = both[:, :gz]
            out_ref[pl.ds(at + 1, probes, stride=planes * gy), :] = both[:, gz:]
            return c

        lax.fori_loop(0, size // 2, pair, 0)

    def send(ch, owner, target, slot):
        plane, y0 = ch // per, (ch % per) * size
        view = out.at[:, plane, pl.ds(pl.multiple_of(owner * own + y0, 8), size), :]
        return pltpu.make_async_remote_copy(
            src_ref=view,
            dst_ref=view,
            send_sem=osend.at[slot, ch],
            recv_sem=orecv.at[slot, ch],
            device_id={"node": target},
            device_id_type=MESH,
        )

    started = []
    if parts == 4:
        near = me + 1 - 2 * lax.rem(me, 2)
        far = lax.rem(me + 2, 4)

        def launch(ch):
            for slot, target in ((0, near), (1, far)):
                copy = send(ch, me, target, slot)
                copy.start()
                started.append(copy)

        respond(0)
        for ch in range(1, chunks):
            respond(ch)
            launch(ch - 1)
        launch(chunks - 1)
        for ch in range(chunks):
            a, b = send(ch, near, near, 0), send(ch, far, far, 1)
            a.wait_recv()
            b.wait_recv()
            copy = send(ch, near, far, 2) if ch % 2 else send(ch, far, near, 2)
            copy.start()
            started.append(copy)
    else:
        for ch in range(chunks):
            respond(ch)
            for d in range(1, parts):
                copy = send(ch, me, lax.rem(me + d, parts), d - 1)
                copy.start()
                started.append(copy)

    gsum_ref[...] = collect(count, row, part_ref, grow_ref, gcopies)
    gncopies = exchange("node", parts, me, gsum_ref, gnode_ref, gnsend, gnrecv)
    diag = collect(parts, me, gsum_ref, gnode_ref, gncopies)
    source = lax.broadcasted_iota(jnp.int32, (nf, cols), 0)
    column = lax.broadcasted_iota(jnp.int32, (nf, cols), 1)
    total = jnp.zeros((cols, cols), jnp.float32)
    for m in range(NODE_DEV):
        node = assign_ref[me * NODE_DEV + m]
        pick = ((source // (2 * cols) == node) & (source % cols == column)).astype(jnp.bfloat16)
        rest = diag
        picked = jnp.zeros((cols, cols), jnp.float32)
        for _ in range(3):
            piece = rest.astype(jnp.bfloat16)
            rest = rest - piece.astype(jnp.float32)
            picked = picked + jnp.dot(piece, pick, preferred_element_type=jnp.float32)
        total = total + weights_ref[node] * picked
    gram_ref[...] = total / cells

    if parts == 4:
        for ch in range(chunks):
            diagonal = lax.rem(near + 2, 4)
            send(ch, diagonal, near, 2).wait_recv()
        for copy in started:
            copy.wait_send()
    else:
        for ch in range(chunks):
            for d in range(1, parts):
                send(ch, lax.rem(me + parts - d, parts), me, d - 1).wait_recv()
        for copy in started:
            copy.wait_send()


def split(v):
    hi = v.astype(jnp.bfloat16)
    return hi, (v - hi.astype(jnp.float32)).astype(jnp.bfloat16)


def local(inputs, diagonal, observations, frequencies, weights, counts, assignment):
    parts = lax.axis_size("node")
    count = lax.axis_size("row")
    cols, planes, gy, gz = inputs.shape
    probes = observations.shape[0]
    quad = frequencies.shape[0]
    own = gy // parts
    halo = ITERS - 1
    win = own + 2 * halo
    size = own + 2 * EDGE
    nf = quad * 2 * cols
    local_rows = planes * own

    total = planes + 2 * halo
    vmem = pl.BlockSpec(memory_space=pltpu.VMEM)
    smem = pl.BlockSpec(memory_space=pltpu.SMEM)
    hbm = pl.BlockSpec(memory_space=pl.ANY)
    dma = pltpu.SemaphoreType.DMA
    src, diag, obs = pl.pallas_call(
        functools.partial(exchange_kernel, halo, own, parts, count),
        out_shape=(
            jax.ShapeDtypeStruct((total, size + 2 * EDGE, cols, gz), jnp.float32),
            jax.ShapeDtypeStruct((total, size, gz), jnp.float32),
            jax.ShapeDtypeStruct((local_rows, probes, gz), jnp.float32),
        ),
        in_specs=[hbm, hbm, hbm],
        out_specs=(vmem, vmem, vmem),
        scratch_shapes=[
            pltpu.VMEM((total, cols, size, gz), jnp.float32),
            pltpu.VMEM((planes, probes, own, gz), jnp.float32),
            dma((planes,)),
            dma,
            dma((planes,)),
            dma((total + 2,)),
            dma((total,)),
            dma((4,)),
            dma((4,)),
        ],
        compiler_params=pltpu.CompilerParams(
            vmem_limit_bytes=EXCHANGE_VMEM, collective_id=1, has_side_effects=True
        ),
        name="exchange",
    )(*[pltpu.with_memory_space_constraint(x, pltpu.HBM) for x in (inputs, diagonal, observations)])

    fhl, proj, diags = pl.pallas_call(
        functools.partial(sweep_kernel, halo, own, planes),
        out_shape=(
            jax.ShapeDtypeStruct((local_rows, 2, quad, 2, cols, gz), jnp.bfloat16),
            jax.ShapeDtypeStruct((probes, nf), jnp.float32),
            jax.ShapeDtypeStruct((cols, nf), jnp.float32),
        ),
        in_specs=[smem, smem, vmem, vmem, vmem],
        out_specs=(vmem, vmem, vmem),
        scratch_shapes=[
            pltpu.VMEM((nf + 2 * probes, 2 * nf), jnp.float32),
            pltpu.VMEM((2, total, win + 6, cols, gz), jnp.float32),
            pltpu.VMEM((2, total, win + 6, cols, gz), jnp.float32),
            pltpu.VMEM((2 * gz, gz), jnp.bfloat16),
            pltpu.VMEM((GROUPS, 2, 2, STEP + 2, cols, gz), jnp.float32),
            pltpu.VMEM((total, size + 2 * EDGE, gz), jnp.float32),
            pltpu.VMEM((total, size + 2 * EDGE, gz), jnp.float32),
        ],
        compiler_params=pltpu.CompilerParams(vmem_limit_bytes=SWEEP_VMEM),
        name="sweeps",
    )(counts, frequencies, obs, src, diag)

    cells = planes * gy * gz * count
    chunks = planes * (own // min(CHUNK, own))
    response, group_gram = pl.pallas_call(
        functools.partial(tail_kernel, parts, count, planes, own, cells),
        out_shape=(
            jax.ShapeDtypeStruct((probes * planes * gy, gz), jnp.float32),
            jax.ShapeDtypeStruct((cols, cols), jnp.float32),
        ),
        in_specs=[smem, smem, vmem, vmem, vmem],
        out_specs=(vmem, vmem),
        scratch_shapes=[
            pltpu.VMEM((count, probes, nf), jnp.float32),
            pltpu.VMEM((probes, nf), jnp.float32),
            pltpu.VMEM((parts, probes, nf), jnp.float32),
            pltpu.VMEM((count, cols, nf), jnp.float32),
            pltpu.VMEM((cols, nf), jnp.float32),
            pltpu.VMEM((parts, cols, nf), jnp.float32),
            dma((count - 1,)),
            dma((count - 1,)),
            dma((parts - 1,)),
            dma((parts - 1,)),
            dma((count - 1,)),
            dma((count - 1,)),
            dma((parts - 1,)),
            dma((parts - 1,)),
            dma((parts - 1, chunks)),
            dma((parts - 1, chunks)),
        ],
        compiler_params=pltpu.CompilerParams(
            vmem_limit_bytes=TAIL_VMEM, collective_id=0, has_side_effects=True
        ),
        name="tail",
    )(weights, assignment, proj, diags, fhl.reshape(local_rows, 2 * nf, gz))
    return response.reshape(probes, planes, gy, gz), group_gram[None]


def solution(mesh):
    placed = (
        P(None, "row", None, None),
        P("row", None, None),
        P(None, "row", None, None),
        P(),
        P(),
        P(),
        P(),
    )
    return jax.shard_map(
        local,
        mesh=mesh,
        in_specs=placed,
        out_specs=(P(None, "row", None, None), P("node", None, None)),
        check_vma=False,
    )
```

```python
import functools

import jax
import jax.numpy as jnp
from jax import lax
from jax.experimental import pallas as pl
from jax.experimental.pallas import tpu as pltpu
from jax.sharding import PartitionSpec as P

NODE_DEV = 1
ITERS = 6
EXCHANGE_VMEM = 8 * 1024 * 1024
SWEEP_VMEM = 30 * 1024 * 1024
TAIL_VMEM = 16 * 1024 * 1024
STEP = 8
OFF = 1
EDGE = 8
GROUPS = 2
MERGE = 2
START = 6
CHUNK = 16
MESH = pl.DeviceIdType.MESH


def exchange_kernel(halo, own, parts, count, inputs, diagonal, observations, src_ref, dg_ref, ob_ref,
                    nat_ref, onat_ref, load_sem, dload_sem, oload_sem, send_sem, recv_sem, dsend_sem, drecv_sem):
    me = lax.axis_index("node")
    row = lax.axis_index("row")
    cols, planes, gy, gz = inputs.shape
    probes = observations.shape[0]
    size = nat_ref.shape[2]
    start = pl.multiple_of(jnp.clip(me * own - EDGE, 0, gy - size), 8)
    top = halo + planes
    last = top + halo - 1

    loads = []
    for j in range(planes):
        loads.append(
            pltpu.make_async_copy(inputs.at[:, j, pl.ds(start, size), :], nat_ref.at[j], load_sem.at[j])
        )
        loads[-1].start()
    dload = pltpu.make_async_copy(
        diagonal.at[:, pl.ds(start, size), :], dg_ref.at[pl.ds(halo, planes)], dload_sem
    )
    dload.start()
    oloads = []
    for j in range(planes):
        rows = pl.ds(pl.multiple_of(me * own, 8), own)
        oloads.append(
            pltpu.make_async_copy(observations.at[:, j, rows, :], onat_ref.at[j], oload_sem.at[j])
        )
        oloads[-1].start()

    barrier = pltpu.get_barrier_semaphore()
    for hop in (-2, -1, 1, 2):
        @pl.when((row + hop >= 0) & (row + hop < count))
        def _():
            pl.semaphore_signal(barrier, inc=1, device_id={"row": row + hop}, device_id_type=MESH)

    def plane(source, target, send, to):
        away = halo - target if target < halo else target - top + 1
        rows = pl.ds(2 * EDGE - halo + away, own + 2 * (halo - away))
        return pltpu.make_async_remote_copy(
            src_ref=src_ref.at[source, rows],
            dst_ref=src_ref.at[target, rows],
            send_sem=send_sem.at[send],
            recv_sem=recv_sem.at[target],
            device_id={"row": to},
            device_id_type=MESH,
        )

    def strip(source, target, size, slot, to):
        return pltpu.make_async_remote_copy(
            src_ref=dg_ref.at[pl.ds(source, size)],
            dst_ref=dg_ref.at[pl.ds(target, size)],
            send_sem=dsend_sem.at[slot],
            recv_sem=drecv_sem.at[slot],
            device_id={"row": to},
            device_id_type=MESH,
        )

    even = lax.rem(row, 2) == 0
    far = halo - planes
    up = [plane(halo + j, far + j, far + j, row + 1) for j in range(planes)]
    up_far = plane(top - 1, 0, 0, row + 2)
    up_pass = plane(halo - 1, 0, last + 1, row + 1)
    down = [plane(halo + j, top + j, top + j, row - 1) for j in range(planes)]
    down_far = plane(halo, last, last, row - 2)
    down_pass = plane(top, last, last + 2, row - 1)
    strips = (
        (row + 1 < count, row >= 1, strip(halo, far, planes, 0, row + 1)),
        (row + 2 < count, row >= 2, strip(top - far, 0, far, 1, row + 2)),
        (row >= 1, row + 1 < count, strip(halo, top, planes, 2, row - 1)),
        (row >= 2, row + 2 < count, strip(halo, top + planes, far, 3, row - 2)),
    )
    has_up, has_down = row + 1 < count, row >= 1
    direct_up, direct_down = even & (row + 2 < count), ~even & (row >= 2)
    pass_up, pass_down = even & has_down & has_up, ~even & has_up & has_down

    def when(flag, *actions):
        @pl.when(flag)
        def _():
            for action in actions:
                action()

    base = start - (me * own - 2 * EDGE)

    def turn(j):
        loads[j].wait()

        def block(o, c):
            at = pl.multiple_of(8 * o, 8)
            for h in range(cols // 8):
                value = nat_ref[j, 8 * h : 8 * h + 8, pl.ds(at, 8), :]
                src_ref[halo + j, pl.ds(base + at, 8), 8 * h : 8 * h + 8, :] = jnp.swapaxes(value, 0, 1)
            return c

        lax.fori_loop(0, size // 8, block, 0)

    def blank(p, at, n):
        src_ref[p, at : at + n] = jnp.zeros((n,) + src_ref.shape[2:], jnp.float32)

    for j in range(planes):
        when(me == 0, lambda: blank(halo + j, EDGE, EDGE))
        when(me == parts - 1, lambda: blank(halo + j, own + 2 * EDGE, EDGE))
    turn(planes - 1)
    turn(0)
    dload.wait()
    pl.semaphore_wait(barrier, jnp.minimum(row, 2) + jnp.minimum(count - 1 - row, 2))
    for n in range(1, planes):
        if n + 1 < planes:
            turn(planes - 1 - n)
        when(has_up, up[planes - n].start)
        when(has_down, down[n - 1].start)
        if n == 1:
            when(direct_up, up_far.start)
            when(direct_down, down_far.start)
            for sends, _, copy in strips:
                when(sends, copy.start)
    when(has_up, up[0].start)
    when(has_down, down[planes - 1].start)

    for away in range(1, halo + 1):
        for p in (halo - away, top - 1 + away):
            blank(p, 2 * EDGE - halo, away)
            blank(p, own + 2 * EDGE + halo - away, away)

    for copy in oloads:
        copy.wait()

    def probe(n, c):
        p, at = n // (own // 8), pl.multiple_of(lax.rem(n, own // 8) * 8, 8)
        for h in range(probes // 8):
            value = jnp.swapaxes(onat_ref[p, 8 * h : 8 * h + 8, pl.ds(at, 8), :], 0, 1)
            ob_ref[pl.ds(8 * n, 8), 8 * h : 8 * h + 8, :] = value
        return c

    lax.fori_loop(0, planes * (own // 8), probe, 0)

    when(has_down, up[-1].wait_recv)
    when(pass_up, up_pass.start)
    when(has_up, down[0].wait_recv)
    when(pass_down, down_pass.start)
    for j in range(1, planes):
        when(has_down, up[planes - 1 - j].wait_recv)
        when(has_up, down[j].wait_recv)
    when(row >= 2, up_far.wait_recv)
    when(row + 2 < count, down_far.wait_recv)
    for _, receives, copy in strips:
        when(receives, copy.wait_recv)

    def clear(at, n):
        def one(p, c):
            src_ref[p] = jnp.zeros(src_ref.shape[1:], jnp.float32)
            dg_ref[p] = jnp.zeros(dg_ref.shape[1:], jnp.float32)
            return c

        return lambda: lax.fori_loop(at, at + n, one, 0)

    when(row < 1, clear(far, planes))
    when(row < 2, clear(0, far))
    when(row + 1 >= count, clear(top, planes))
    when(row + 2 >= count, clear(top + planes, far))

    when(has_up, *[copy.wait_send for copy in up])
    when(has_down, *[copy.wait_send for copy in down])
    when(direct_up, up_far.wait_send)
    when(direct_down, down_far.wait_send)
    when(pass_up, up_pass.wait_send)
    when(pass_down, down_pass.wait_send)
    for sends, _, copy in strips:
        when(sends, copy.wait_send)


def sweep_kernel(halo, own, planes, counts_ref, freq_ref, obs_ref, src_ref, dg_ref, fhl_ref, proj_ref, gram_ref,
                 acc_ref, xa_ref, xb_ref, near_ref, st_ref, gr_ref, gi_ref):
    total = planes + 2 * halo
    cols, gz = src_ref.shape[2:]
    quad = counts_ref.shape[0]
    size = dg_ref.shape[1]
    me = lax.axis_index("node")
    start = jnp.clip(me * own - EDGE, 0, own * lax.axis_size("node") - size)
    lift = me * own - halo - OFF - start + EDGE
    skew = 2 * EDGE - halo - OFF

    gap = lax.broadcasted_iota(jnp.int32, (2 * gz, gz), 0) % gz - lax.broadcasted_iota(
        jnp.int32, (2 * gz, gz), 1
    )
    near_ref[...] = ((gap == 1) | (gap == -1)).astype(jnp.bfloat16)
    lane = lax.broadcasted_iota(jnp.int32, (cols, gz), 1)
    first = lane == 0
    last = lane == gz - 1

    def beside(v):
        return jnp.where(first, 0.0, pltpu.roll(v, 1, 1)) + jnp.where(
            last, 0.0, pltpu.roll(v, gz - 1, 1)
        )

    def gain(p, y):
        return (
            jnp.broadcast_to(gr_ref[p, pl.ds(y + lift, 1), :], (cols, gz)),
            jnp.broadcast_to(gi_ref[p, pl.ds(y + lift, 1), :], (cols, gz)),
        )

    def stage(x_ref, spots, parity):
        for g, (p, y) in enumerate(spots):
            us = [[x_ref[0, p + q, y - 1 + t] for t in range(STEP + 2)] for q in range(2)]
            for t in range(STEP):
                for q in range(2):
                    n = (us[q][t] + us[q][t + 2]) + (us[1 - q][t + 1] + src_ref[p + q, y + skew + t])
                    st_ref[g, 0, q, parity + t] = n + beside(us[q][t + 1])
        left, sums = [], []
        for g, (p, y) in enumerate(spots):
            ws = [[x_ref[1, p + q, y - 1 + t] for t in range(STEP + 2)] for q in range(2)]
            for t in range(STEP):
                for q in range(2):
                    hi, lo = split(ws[q][t + 1])
                    left.append(jnp.concatenate([hi, lo], 1))
        z = jnp.dot(jnp.concatenate(left, 0), near_ref[...], preferred_element_type=jnp.float32)
        for g, (p, y) in enumerate(spots):
            ws = [[x_ref[1, p + q, y - 1 + t] for t in range(STEP + 2)] for q in range(2)]
            for t in range(STEP):
                for q in range(2):
                    n = (ws[q][t] + ws[q][t + 2]) + ws[1 - q][t + 1]
                    at = (2 * (STEP * g + t) + q) * cols
                    st_ref[g, 1, q, parity + t] = n + z[at : at + cols]

    def combine(x_ref, spots, put, parity):
        for g, (p, y) in enumerate(spots):
            for t in range(STEP):
                for q in range(2):
                    side = p + 3 * q - 1
                    nu = st_ref[g, 0, q, parity + t] + x_ref[0, side, y + t]
                    nw = st_ref[g, 1, q, parity + t] + x_ref[1, side, y + t]
                    gr, gi = gain(p + q, y + t)
                    put(p + q, y + t, gr * nu - gi * nw, gr * nw + gi * nu)

    def sweep(x_ref, radius, put):
        first_plane = halo - radius
        low = first_plane + OFF
        parity = lax.rem(low, 2)
        groups = (own + 2 * radius + STEP - 1) // STEP
        end = low + STEP * groups
        top = first_plane + planes + 2 * radius - 2
        pairs = (planes + 2 * radius) // 2

        def after(p, y):
            wrap = y + STEP >= end
            past = p + 2 > top
            ny = jnp.where(wrap, jnp.where(past, y, low), y + STEP)
            return jnp.where(wrap & ~past, p + 2, p), ny

        spots = [(first_plane, low)]
        for _ in range(GROUPS - 1):
            spots.append(after(*spots[-1]))
        stage(x_ref, spots, parity)

        def body(j, spots):
            nxt = [after(*spots[-1])]
            for _ in range(GROUPS - 1):
                nxt.append(after(*nxt[-1]))
            combine(x_ref, spots, put, parity)
            stage(x_ref, nxt, parity)
            return tuple(nxt)

        lax.fori_loop(0, (groups * pairs + GROUPS - 1) // GROUPS, body, tuple(spots))

    def node(k, c):
        w = freq_ref[k]
        count = counts_ref[k]
        low1 = halo + 1 - count

        def gains(p, c):
            part = dg_ref[p]
            d = 6.0 + part
            inv = jnp.where(part > 0.0, 1.0 / (d * d + w * w), 0.0)
            rows = slice(EDGE, EDGE + size)
            for ref, value in ((gr_ref, d * inv), (gi_ref, -w * inv)):
                ref[p, :EDGE] = jnp.zeros((EDGE, gz), jnp.float32)
                ref[p, rows] = value
                ref[p, EDGE + size :] = jnp.zeros((EDGE, gz), jnp.float32)
            return c

        lax.fori_loop(low1, total - low1, gains, 0)

        groups1 = (own + 2 * (count - 1) + START - 1) // START

        def start_plane(p, c):
            def rows(j, c):
                y = low1 + OFF + START * j
                for t in range(START):
                    b = src_ref[p, y + skew + t]
                    gr, gi = gain(p, y + t)
                    xa_ref[0, p, y + t] = gr * b
                    xa_ref[1, p, y + t] = gi * b
                return c

            return lax.fori_loop(0, groups1, rows, c)

        lax.fori_loop(low1, low1 + planes + 2 * (count - 1), start_plane, 0)

        def into(ref):
            def put(p, y, u, v):
                ref[0, p, y] = u
                ref[1, p, y] = v

            return put

        def put_last(p, y, u, v):
            row = (p - halo) * own + (y - halo - OFF)
            for comp, value in ((0, u), (1, v)):
                hi, lo = split(value)
                fhl_ref[row, 0, k, comp] = hi
                fhl_ref[row, 1, k, comp] = lo

        inner = count - 2

        def pair(i, c):
            s = 2 * i + 2
            sweep(xa_ref, count - s, into(xb_ref))

            @pl.when(2 * i + 1 < inner)
            def _():
                sweep(xb_ref, count - s - 1, into(xa_ref))

            return c

        lax.fori_loop(0, (inner + 1) // 2, pair, 0)

        @pl.when(inner % 2 == 1)
        def _():
            sweep(xb_ref, 0, put_last)

        @pl.when(inner % 2 == 0)
        def _():
            sweep(xa_ref, 0, put_last)

        return c

    lax.fori_loop(0, quad, node, 0)

    nf = quad * 2 * cols
    acc_ref[...] = jnp.zeros_like(acc_ref)

    def products(j, c):
        total = None
        for m in range(MERGE):
            his, los, ohis, olos = [], [], [], []
            for t in range(2):
                row = 2 * (MERGE * j + m) + t
                his.append(fhl_ref[row, 0].reshape(nf, gz))
                los.append(fhl_ref[row, 1].reshape(nf, gz))
                ohi, olo = split(obs_ref[row])
                ohis.append(ohi)
                olos.append(olo)
            hi = jnp.concatenate(his, 1)
            left = jnp.concatenate([hi, jnp.concatenate(ohis, 1), jnp.concatenate(olos, 1)], 0)
            right = jnp.concatenate([hi, jnp.concatenate(los, 1)], 0)
            part = lax.dot_general(
                left, right, (((1,), (1,)), ((), ())), preferred_element_type=jnp.float32
            )
            total = part if total is None else total + part
        acc_ref[...] += total
        return c

    lax.fori_loop(0, fhl_ref.shape[0] // (2 * MERGE), products, 0)

    probes = obs_ref.shape[1]
    proj_ref[...] = (
        acc_ref[nf : nf + probes, :nf] + acc_ref[nf + probes :, :nf] + acc_ref[nf : nf + probes, nf:]
    )
    cross = acc_ref[:nf, nf:]
    gram = acc_ref[:nf, :nf] + cross + cross.T
    block = lax.broadcasted_iota(jnp.int32, (cols, nf), 1) // cols
    diag = jnp.zeros((cols, nf), jnp.float32)
    for n in range(nf // cols):
        diag = diag + jnp.where(block == n, gram[n * cols : (n + 1) * cols], 0.0)
    gram_ref[...] = diag


def tail_kernel(parts, count, planes, own, cells, weights_ref, assign_ref, proj_ref, part_ref, f_ref,
                out_ref, gram_ref, prow_ref, psum_ref, pnode_ref, grow_ref, gsum_ref, gnode_ref,
                psend, precv, pnsend, pnrecv, gsend, grecv, gnsend, gnrecv, osend, orecv):
    me = lax.axis_index("node")
    row = lax.axis_index("row")
    probes, nf = proj_ref.shape
    cols = part_ref.shape[0]
    quad = weights_ref.shape[0]
    gz = out_ref.shape[1]
    gy = own * parts
    out = out_ref.reshape(probes, planes, gy, gz)

    barrier = pltpu.get_barrier_semaphore()
    for d in range(1, count):
        pl.semaphore_signal(barrier, inc=1, device_id={"row": lax.rem(row + d, count)}, device_id_type=MESH)
    for d in range(1, parts):
        pl.semaphore_signal(barrier, inc=1, device_id={"node": lax.rem(me + d, parts)}, device_id_type=MESH)
    pl.semaphore_wait(barrier, count - 1 + parts - 1)

    def exchange(axis, size, index, src, buf, send, recv):
        copies = []
        for d in range(1, size):
            copies.append(
                pltpu.make_async_remote_copy(
                    src_ref=src,
                    dst_ref=buf.at[index],
                    send_sem=send.at[d - 1],
                    recv_sem=recv.at[d - 1],
                    device_id={axis: lax.rem(index + d, size)},
                    device_id_type=MESH,
                )
            )
            copies[-1].start()
        return copies

    def collect(size, index, src, buf, copies):
        buf[index] = src[...]
        for copy in copies:
            copy.wait()
        total = buf[0]
        for n in range(1, size):
            total = total + buf[n]
        return total

    pcopies = exchange("row", count, row, proj_ref, prow_ref, psend, precv)
    psum_ref[...] = collect(count, row, proj_ref, prow_ref, pcopies)
    pncopies = exchange("node", parts, me, psum_ref, pnode_ref, pnsend, pnrecv)
    gcopies = exchange("row", count, row, part_ref, grow_ref, gsend, grecv)
    proj = collect(parts, me, psum_ref, pnode_ref, pncopies)

    lane = lax.broadcasted_iota(jnp.int32, (1, nf), 1) // (2 * cols)
    scale = jnp.zeros((1, nf), jnp.float32)
    for k in range(quad):
        scale = jnp.where(lane == k, weights_ref[k] / quad, scale)
    hi, lo = split(proj * scale)
    pw = jnp.concatenate(
        [jnp.concatenate([hi, hi], 1), jnp.concatenate([lo, jnp.zeros_like(lo)], 1)], 0
    )

    size = min(CHUNK, own)
    per = own // size
    chunks = planes * per

    def respond(ch):
        plane, y0 = ch // per, (ch % per) * size

        def pair(j, c):
            r = plane * own + y0 + 2 * j
            right = jnp.concatenate([f_ref[r], f_ref[r + 1]], 1)
            both = jnp.dot(pw, right, preferred_element_type=jnp.float32)
            both = both[:probes] + both[probes:]
            at = plane * gy + me * own + y0 + 2 * j
            out_ref[pl.ds(at, probes, stride=planes * gy), :] = both[:, :gz]
            out_ref[pl.ds(at + 1, probes, stride=planes * gy), :] = both[:, gz:]
            return c

        lax.fori_loop(0, size // 2, pair, 0)

    def send(ch, owner, target, slot):
        plane, y0 = ch // per, (ch % per) * size
        view = out.at[:, plane, pl.ds(pl.multiple_of(owner * own + y0, 8), size), :]
        return pltpu.make_async_remote_copy(
            src_ref=view,
            dst_ref=view,
            send_sem=osend.at[slot, ch],
            recv_sem=orecv.at[slot, ch],
            device_id={"node": target},
            device_id_type=MESH,
        )

    def spread():
        gsum_ref[...] = collect(count, row, part_ref, grow_ref, gcopies)
        return exchange("node", parts, me, gsum_ref, gnode_ref, gnsend, gnrecv)

    started = []
    if parts == 4:
        near = me + 1 - 2 * lax.rem(me, 2)
        far = lax.rem(me + 2, 4)

        def launch(ch):
            for slot, target in ((0, near), (1, far)):
                copy = send(ch, me, target, slot)
                copy.start()
                started.append(copy)

        respond(0)
        for ch in range(1, chunks):
            respond(ch)
            launch(ch - 1)
        launch(chunks - 1)
        gncopies = spread()
        for ch in range(chunks):
            a, b = send(ch, near, near, 0), send(ch, far, far, 1)
            a.wait_recv()
            b.wait_recv()
            copy = send(ch, near, far, 2) if ch % 2 else send(ch, far, near, 2)
            copy.start()
            started.append(copy)
    else:
        for ch in range(chunks):
            respond(ch)
            for d in range(1, parts):
                copy = send(ch, me, lax.rem(me + d, parts), d - 1)
                copy.start()
                started.append(copy)

    if parts != 4:
        gncopies = spread()
    diag = collect(parts, me, gsum_ref, gnode_ref, gncopies)
    source = lax.broadcasted_iota(jnp.int32, (nf, cols), 0)
    column = lax.broadcasted_iota(jnp.int32, (nf, cols), 1)
    total = jnp.zeros((cols, cols), jnp.float32)
    for m in range(NODE_DEV):
        node = assign_ref[me * NODE_DEV + m]
        pick = ((source // (2 * cols) == node) & (source % cols == column)).astype(jnp.bfloat16)
        rest = diag
        picked = jnp.zeros((cols, cols), jnp.float32)
        for _ in range(3):
            piece = rest.astype(jnp.bfloat16)
            rest = rest - piece.astype(jnp.float32)
            picked = picked + jnp.dot(piece, pick, preferred_element_type=jnp.float32)
        total = total + weights_ref[node] * picked
    gram_ref[...] = total / cells

    if parts == 4:
        for ch in range(chunks):
            diagonal = lax.rem(near + 2, 4)
            send(ch, diagonal, near, 2).wait_recv()
        for copy in started:
            copy.wait_send()
    else:
        for ch in range(chunks):
            for d in range(1, parts):
                send(ch, lax.rem(me + parts - d, parts), me, d - 1).wait_recv()
        for copy in started:
            copy.wait_send()


def split(v):
    hi = v.astype(jnp.bfloat16)
    return hi, (v - hi.astype(jnp.float32)).astype(jnp.bfloat16)


def local(inputs, diagonal, observations, frequencies, weights, counts, assignment):
    parts = lax.axis_size("node")
    count = lax.axis_size("row")
    cols, planes, gy, gz = inputs.shape
    probes = observations.shape[0]
    quad = frequencies.shape[0]
    own = gy // parts
    halo = ITERS - 1
    win = own + 2 * halo
    size = own + 2 * EDGE
    nf = quad * 2 * cols
    local_rows = planes * own

    total = planes + 2 * halo
    vmem = pl.BlockSpec(memory_space=pltpu.VMEM)
    smem = pl.BlockSpec(memory_space=pltpu.SMEM)
    hbm = pl.BlockSpec(memory_space=pl.ANY)
    dma = pltpu.SemaphoreType.DMA
    src, diag, obs = pl.pallas_call(
        functools.partial(exchange_kernel, halo, own, parts, count),
        out_shape=(
            jax.ShapeDtypeStruct((total, size + 2 * EDGE, cols, gz), jnp.float32),
            jax.ShapeDtypeStruct((total, size, gz), jnp.float32),
            jax.ShapeDtypeStruct((local_rows, probes, gz), jnp.float32),
        ),
        in_specs=[hbm, hbm, hbm],
        out_specs=(vmem, vmem, vmem),
        scratch_shapes=[
            pltpu.VMEM((planes, cols, size, gz), jnp.float32),
            pltpu.VMEM((planes, probes, own, gz), jnp.float32),
            dma((planes,)),
            dma,
            dma((planes,)),
            dma((total + 2,)),
            dma((total,)),
            dma((4,)),
            dma((4,)),
        ],
        compiler_params=pltpu.CompilerParams(
            vmem_limit_bytes=EXCHANGE_VMEM, collective_id=1, has_side_effects=True
        ),
        name="exchange",
    )(*[pltpu.with_memory_space_constraint(x, pltpu.HBM) for x in (inputs, diagonal, observations)])

    fhl, proj, diags = pl.pallas_call(
        functools.partial(sweep_kernel, halo, own, planes),
        out_shape=(
            jax.ShapeDtypeStruct((local_rows, 2, quad, 2, cols, gz), jnp.bfloat16),
            jax.ShapeDtypeStruct((probes, nf), jnp.float32),
            jax.ShapeDtypeStruct((cols, nf), jnp.float32),
        ),
        in_specs=[smem, smem, vmem, vmem, vmem],
        out_specs=(vmem, vmem, vmem),
        scratch_shapes=[
            pltpu.VMEM((nf + 2 * probes, 2 * nf), jnp.float32),
            pltpu.VMEM((2, total, win + 6, cols, gz), jnp.float32),
            pltpu.VMEM((2, total, win + 6, cols, gz), jnp.float32),
            pltpu.VMEM((2 * gz, gz), jnp.bfloat16),
            pltpu.VMEM((GROUPS, 2, 2, STEP + 2, cols, gz), jnp.float32),
            pltpu.VMEM((total, size + 2 * EDGE, gz), jnp.float32),
            pltpu.VMEM((total, size + 2 * EDGE, gz), jnp.float32),
        ],
        compiler_params=pltpu.CompilerParams(vmem_limit_bytes=SWEEP_VMEM),
        name="sweeps",
    )(counts, frequencies, obs, src, diag)

    cells = planes * gy * gz * count
    chunks = planes * (own // min(CHUNK, own))
    response, group_gram = pl.pallas_call(
        functools.partial(tail_kernel, parts, count, planes, own, cells),
        out_shape=(
            jax.ShapeDtypeStruct((probes * planes * gy, gz), jnp.float32),
            jax.ShapeDtypeStruct((cols, cols), jnp.float32),
        ),
        in_specs=[smem, smem, vmem, vmem, vmem],
        out_specs=(vmem, vmem),
        scratch_shapes=[
            pltpu.VMEM((count, probes, nf), jnp.float32),
            pltpu.VMEM((probes, nf), jnp.float32),
            pltpu.VMEM((parts, probes, nf), jnp.float32),
            pltpu.VMEM((count, cols, nf), jnp.float32),
            pltpu.VMEM((cols, nf), jnp.float32),
            pltpu.VMEM((parts, cols, nf), jnp.float32),
            dma((count - 1,)),
            dma((count - 1,)),
            dma((parts - 1,)),
            dma((parts - 1,)),
            dma((count - 1,)),
            dma((count - 1,)),
            dma((parts - 1,)),
            dma((parts - 1,)),
            dma((parts - 1, chunks)),
            dma((parts - 1, chunks)),
        ],
        compiler_params=pltpu.CompilerParams(
            vmem_limit_bytes=TAIL_VMEM, collective_id=0, has_side_effects=True
        ),
        name="tail",
    )(weights, assignment, proj, diags, fhl.reshape(local_rows, 2 * nf, gz))
    return response.reshape(probes, planes, gy, gz), group_gram[None]


def solution(mesh):
    placed = (
        P(None, "row", None, None),
        P("row", None, None),
        P(None, "row", None, None),
        P(),
        P(),
        P(),
        P(),
    )
    return jax.shard_map(
        local,
        mesh=mesh,
        in_specs=placed,
        out_specs=(P(None, "row", None, None), P("node", None, None)),
        check_vma=False,
    )
```

```python
import functools

import jax
import jax.numpy as jnp
from jax import lax
from jax.experimental import pallas as pl
from jax.experimental.pallas import tpu as pltpu
from jax.sharding import PartitionSpec as P

NODE_DEV = 1
ITERS = 6
EXCHANGE_VMEM = 8 * 1024 * 1024
SWEEP_VMEM = 30 * 1024 * 1024
TAIL_VMEM = 16 * 1024 * 1024
STEP = 8
OFF = 1
EDGE = 8
GROUPS = 2
MERGE = 2
SPAN = 8
START = 6
CHUNK = 8
MESH = pl.DeviceIdType.MESH


def exchange_kernel(halo, own, parts, count, inputs, diagonal, observations, src_ref, dg_ref, ob_ref,
                    nat_ref, onat_ref, load_sem, dload_sem, oload_sem, send_sem, recv_sem, dsend_sem, drecv_sem):
    me = lax.axis_index("node")
    row = lax.axis_index("row")
    cols, planes, gy, gz = inputs.shape
    probes = observations.shape[0]
    size = nat_ref.shape[2]
    start = pl.multiple_of(jnp.clip(me * own - EDGE, 0, gy - size), 8)
    top = halo + planes
    last = top + halo - 1

    loads = []
    for j in range(planes):
        loads.append(
            pltpu.make_async_copy(inputs.at[:, j, pl.ds(start, size), :], nat_ref.at[j], load_sem.at[j])
        )
        loads[-1].start()
    dload = pltpu.make_async_copy(
        diagonal.at[:, pl.ds(start, size), :], dg_ref.at[pl.ds(halo, planes)], dload_sem
    )
    dload.start()
    oloads = []
    for j in range(planes):
        rows = pl.ds(pl.multiple_of(me * own, 8), own)
        oloads.append(
            pltpu.make_async_copy(observations.at[:, j, rows, :], onat_ref.at[j], oload_sem.at[j])
        )
        oloads[-1].start()

    barrier = pltpu.get_barrier_semaphore()
    for hop in (-2, -1, 1, 2):
        @pl.when((row + hop >= 0) & (row + hop < count))
        def _():
            pl.semaphore_signal(barrier, inc=1, device_id={"row": row + hop}, device_id_type=MESH)

    def plane(source, target, send, to):
        away = halo - target if target < halo else target - top + 1
        rows = pl.ds(2 * EDGE - halo + away, own + 2 * (halo - away))
        return pltpu.make_async_remote_copy(
            src_ref=src_ref.at[source, rows],
            dst_ref=src_ref.at[target, rows],
            send_sem=send_sem.at[send],
            recv_sem=recv_sem.at[target],
            device_id={"row": to},
            device_id_type=MESH,
        )

    def strip(source, target, size, slot, to):
        return pltpu.make_async_remote_copy(
            src_ref=dg_ref.at[pl.ds(source, size)],
            dst_ref=dg_ref.at[pl.ds(target, size)],
            send_sem=dsend_sem.at[slot],
            recv_sem=drecv_sem.at[slot],
            device_id={"row": to},
            device_id_type=MESH,
        )

    even = lax.rem(row, 2) == 0
    far = halo - planes
    up = [plane(halo + j, far + j, far + j, row + 1) for j in range(planes)]
    up_far = plane(top - 1, 0, 0, row + 2)
    up_pass = plane(halo - 1, 0, last + 1, row + 1)
    down = [plane(halo + j, top + j, top + j, row - 1) for j in range(planes)]
    down_far = plane(halo, last, last, row - 2)
    down_pass = plane(top, last, last + 2, row - 1)
    strips = (
        (row + 1 < count, row >= 1, strip(halo, far, planes, 0, row + 1)),
        (row + 2 < count, row >= 2, strip(top - far, 0, far, 1, row + 2)),
        (row >= 1, row + 1 < count, strip(halo, top, planes, 2, row - 1)),
        (row >= 2, row + 2 < count, strip(halo, top + planes, far, 3, row - 2)),
    )
    has_up, has_down = row + 1 < count, row >= 1
    direct_up, direct_down = even & (row + 2 < count), ~even & (row >= 2)
    pass_up, pass_down = even & has_down & has_up, ~even & has_up & has_down

    def when(flag, *actions):
        @pl.when(flag)
        def _():
            for action in actions:
                action()

    base = start - (me * own - 2 * EDGE)

    def turn(j):
        loads[j].wait()

        def block(o, c):
            at = pl.multiple_of(8 * o, 8)
            for h in range(cols // 8):
                value = nat_ref[j, 8 * h : 8 * h + 8, pl.ds(at, 8), :]
                src_ref[halo + j, pl.ds(base + at, 8), 8 * h : 8 * h + 8, :] = jnp.swapaxes(value, 0, 1)
            return c

        lax.fori_loop(0, size // 8, block, 0)

    def blank(p, at, n):
        src_ref[p, at : at + n] = jnp.zeros((n,) + src_ref.shape[2:], jnp.float32)

    for j in range(planes):
        when(me == 0, lambda: blank(halo + j, EDGE, EDGE))
        when(me == parts - 1, lambda: blank(halo + j, own + 2 * EDGE, EDGE))
    turn(planes - 1)
    turn(0)
    dload.wait()
    pl.semaphore_wait(barrier, jnp.minimum(row, 2) + jnp.minimum(count - 1 - row, 2))
    for n in range(1, planes):
        if n + 1 < planes:
            turn(planes - 1 - n)
        when(has_up, up[planes - n].start)
        when(has_down, down[n - 1].start)
        if n == 1:
            when(direct_up, up_far.start)
            when(direct_down, down_far.start)
            for sends, _, copy in strips:
                when(sends, copy.start)
    when(has_up, up[0].start)
    when(has_down, down[planes - 1].start)

    for away in range(1, halo + 1):
        for p in (halo - away, top - 1 + away):
            blank(p, 2 * EDGE - halo, away)
            blank(p, own + 2 * EDGE + halo - away, away)

    for copy in oloads:
        copy.wait()

    def probe(n, c):
        p, at = n // (own // 8), pl.multiple_of(lax.rem(n, own // 8) * 8, 8)
        for h in range(probes // 8):
            value = jnp.swapaxes(onat_ref[p, 8 * h : 8 * h + 8, pl.ds(at, 8), :], 0, 1)
            ob_ref[pl.ds(8 * n, 8), 8 * h : 8 * h + 8, :] = value
        return c

    lax.fori_loop(0, planes * (own // 8), probe, 0)

    when(has_down, up[-1].wait_recv)
    when(pass_up, up_pass.start)
    when(has_up, down[0].wait_recv)
    when(pass_down, down_pass.start)
    for j in range(1, planes):
        when(has_down, up[planes - 1 - j].wait_recv)
        when(has_up, down[j].wait_recv)
    when(row >= 2, up_far.wait_recv)
    when(row + 2 < count, down_far.wait_recv)
    for _, receives, copy in strips:
        when(receives, copy.wait_recv)

    def clear(at, n):
        def one(p, c):
            src_ref[p] = jnp.zeros(src_ref.shape[1:], jnp.float32)
            dg_ref[p] = jnp.zeros(dg_ref.shape[1:], jnp.float32)
            return c

        return lambda: lax.fori_loop(at, at + n, one, 0)

    when(row < 1, clear(far, planes))
    when(row < 2, clear(0, far))
    when(row + 1 >= count, clear(top, planes))
    when(row + 2 >= count, clear(top + planes, far))

    when(has_up, *[copy.wait_send for copy in up])
    when(has_down, *[copy.wait_send for copy in down])
    when(direct_up, up_far.wait_send)
    when(direct_down, down_far.wait_send)
    when(pass_up, up_pass.wait_send)
    when(pass_down, down_pass.wait_send)
    for sends, _, copy in strips:
        when(sends, copy.wait_send)


def sweep_kernel(halo, own, planes, counts_ref, freq_ref, src_ref, dg_ref, fhl_ref,
                 xa_ref, xb_ref, near_ref, st_ref, gr_ref, gi_ref):
    total = planes + 2 * halo
    cols, gz = src_ref.shape[2:]
    quad = counts_ref.shape[0]
    size = dg_ref.shape[1]
    me = lax.axis_index("node")
    start = jnp.clip(me * own - EDGE, 0, own * lax.axis_size("node") - size)
    lift = me * own - halo - OFF - start + EDGE
    skew = 2 * EDGE - halo - OFF

    gap = lax.broadcasted_iota(jnp.int32, (2 * gz, gz), 0) % gz - lax.broadcasted_iota(
        jnp.int32, (2 * gz, gz), 1
    )
    near_ref[...] = ((gap == 1) | (gap == -1)).astype(jnp.bfloat16)
    lane = lax.broadcasted_iota(jnp.int32, (cols, gz), 1)
    first = lane == 0
    last = lane == gz - 1

    def beside(v):
        return jnp.where(first, 0.0, pltpu.roll(v, 1, 1)) + jnp.where(
            last, 0.0, pltpu.roll(v, gz - 1, 1)
        )

    def gain(p, y):
        return (
            jnp.broadcast_to(gr_ref[p, pl.ds(y + lift, 1), :], (cols, gz)),
            jnp.broadcast_to(gi_ref[p, pl.ds(y + lift, 1), :], (cols, gz)),
        )

    def stage(x_ref, spots, parity):
        for g, (p, y) in enumerate(spots):
            us = [[x_ref[0, p + q, y - 1 + t] for t in range(STEP + 2)] for q in range(2)]
            for t in range(STEP):
                for q in range(2):
                    n = (us[q][t] + us[q][t + 2]) + (us[1 - q][t + 1] + src_ref[p + q, y + skew + t])
                    st_ref[g, 0, q, parity + t] = n + beside(us[q][t + 1])
        left, sums = [], []
        for g, (p, y) in enumerate(spots):
            ws = [[x_ref[1, p + q, y - 1 + t] for t in range(STEP + 2)] for q in range(2)]
            for t in range(STEP):
                for q in range(2):
                    hi, lo = split(ws[q][t + 1])
                    left.append(jnp.concatenate([hi, lo], 1))
        z = jnp.dot(jnp.concatenate(left, 0), near_ref[...], preferred_element_type=jnp.float32)
        for g, (p, y) in enumerate(spots):
            ws = [[x_ref[1, p + q, y - 1 + t] for t in range(STEP + 2)] for q in range(2)]
            for t in range(STEP):
                for q in range(2):
                    n = (ws[q][t] + ws[q][t + 2]) + ws[1 - q][t + 1]
                    at = (2 * (STEP * g + t) + q) * cols
                    st_ref[g, 1, q, parity + t] = n + z[at : at + cols]

    def combine(x_ref, spots, put, parity):
        for g, (p, y) in enumerate(spots):
            for t in range(STEP):
                for q in range(2):
                    side = p + 3 * q - 1
                    nu = st_ref[g, 0, q, parity + t] + x_ref[0, side, y + t]
                    nw = st_ref[g, 1, q, parity + t] + x_ref[1, side, y + t]
                    gr, gi = gain(p + q, y + t)
                    put(p + q, y + t, gr * nu - gi * nw, gr * nw + gi * nu)

    def sweep(x_ref, radius, put):
        first_plane = halo - radius
        low = first_plane + OFF
        parity = lax.rem(low, 2)
        groups = (own + 2 * radius + STEP - 1) // STEP
        end = low + STEP * groups
        top = first_plane + planes + 2 * radius - 2
        pairs = (planes + 2 * radius) // 2

        def after(p, y):
            wrap = y + STEP >= end
            past = p + 2 > top
            ny = jnp.where(wrap, jnp.where(past, y, low), y + STEP)
            return jnp.where(wrap & ~past, p + 2, p), ny

        spots = [(first_plane, low)]
        for _ in range(GROUPS - 1):
            spots.append(after(*spots[-1]))
        stage(x_ref, spots, parity)

        def body(j, spots):
            nxt = [after(*spots[-1])]
            for _ in range(GROUPS - 1):
                nxt.append(after(*nxt[-1]))
            combine(x_ref, spots, put, parity)
            stage(x_ref, nxt, parity)
            return tuple(nxt)

        lax.fori_loop(0, (groups * pairs + GROUPS - 1) // GROUPS, body, tuple(spots))

    def node(k, c):
        w = freq_ref[k]
        count = counts_ref[k]
        low1 = halo + 1 - count

        def gains(p, c):
            part = dg_ref[p]
            d = 6.0 + part
            inv = jnp.where(part > 0.0, 1.0 / (d * d + w * w), 0.0)
            rows = slice(EDGE, EDGE + size)
            for ref, value in ((gr_ref, d * inv), (gi_ref, -w * inv)):
                ref[p, :EDGE] = jnp.zeros((EDGE, gz), jnp.float32)
                ref[p, rows] = value
                ref[p, EDGE + size :] = jnp.zeros((EDGE, gz), jnp.float32)
            return c

        lax.fori_loop(low1, total - low1, gains, 0)

        groups1 = (own + 2 * (count - 1) + START - 1) // START

        def start_plane(p, c):
            def rows(j, c):
                y = low1 + OFF + START * j
                for t in range(START):
                    b = src_ref[p, y + skew + t]
                    gr, gi = gain(p, y + t)
                    xa_ref[0, p, y + t] = gr * b
                    xa_ref[1, p, y + t] = gi * b
                return c

            return lax.fori_loop(0, groups1, rows, c)

        lax.fori_loop(low1, low1 + planes + 2 * (count - 1), start_plane, 0)

        def into(ref):
            def put(p, y, u, v):
                ref[0, p, y] = u
                ref[1, p, y] = v

            return put

        def put_last(p, y, u, v):
            row = (p - halo) * own + (y - halo - OFF)
            for comp, value in ((0, u), (1, v)):
                hi, lo = split(value)
                fhl_ref[row, 0, k, comp] = hi
                fhl_ref[row, 1, k, comp] = lo

        inner = count - 2

        def pair(i, c):
            s = 2 * i + 2
            sweep(xa_ref, count - s, into(xb_ref))

            @pl.when(2 * i + 1 < inner)
            def _():
                sweep(xb_ref, count - s - 1, into(xa_ref))

            return c

        lax.fori_loop(0, (inner + 1) // 2, pair, 0)

        @pl.when(inner % 2 == 1)
        def _():
            sweep(xb_ref, 0, put_last)

        @pl.when(inner % 2 == 0)
        def _():
            sweep(xa_ref, 0, put_last)

        return c

    lax.fori_loop(0, quad, node, 0)


def tail_kernel(parts, count, planes, own, cells, weights_ref, assign_ref, obs_ref, f_ref,
                out_ref, gram_ref, acc_ref, pt_ref, proj_ref, part_ref, prow_ref, psum_ref, pnode_ref, grow_ref, gsum_ref, gnode_ref,
                psend, precv, pnsend, pnrecv, gsend, grecv, gnsend, gnrecv, osend, orecv):
    me = lax.axis_index("node")
    row = lax.axis_index("row")
    probes, nf = proj_ref.shape
    cols = part_ref.shape[0]
    quad = weights_ref.shape[0]
    gz = out_ref.shape[1]
    gy = own * parts
    out = out_ref.reshape(probes, planes, gy, gz)

    barrier = pltpu.get_barrier_semaphore()
    for d in range(1, count):
        pl.semaphore_signal(barrier, inc=1, device_id={"row": lax.rem(row + d, count)}, device_id_type=MESH)
    for d in range(1, parts):
        pl.semaphore_signal(barrier, inc=1, device_id={"node": lax.rem(me + d, parts)}, device_id_type=MESH)

    def pairs(j):
        r = 2 * j
        return jnp.concatenate([f_ref[r], f_ref[r + 1]], 1)

    def nt(left, right):
        return lax.dot_general(left, right, (((1,), (1,)), ((), ())), preferred_element_type=jnp.float32)

    def probe(n):
        his, los = zip(split(obs_ref[2 * n]), split(obs_ref[2 * n + 1]))
        return jnp.concatenate([jnp.concatenate(his, 1), jnp.concatenate(los, 1)], 0)

    def project(j, c):
        n = SPAN * j
        left = jnp.concatenate([pairs(n + m) for m in range(SPAN)], 1)
        pt_ref[...] += nt(left, jnp.concatenate([probe(n + m) for m in range(SPAN)], 1))
        return c

    steps = f_ref.shape[0] // (2 * MERGE)
    pt_ref[...] = jnp.zeros_like(pt_ref)
    lax.fori_loop(0, f_ref.shape[0] // (2 * SPAN), project, 0)
    both = pt_ref[...].T
    proj_ref[...] = both[:probes, :nf] + both[probes:, :nf] + both[:probes, nf:]
    acc_ref[...] = jnp.zeros_like(acc_ref)
    pl.semaphore_wait(barrier, count - 1 + parts - 1)

    def exchange(axis, size, index, src, buf, send, recv):
        copies = []
        for d in range(1, size):
            copies.append(
                pltpu.make_async_remote_copy(
                    src_ref=src,
                    dst_ref=buf.at[index],
                    send_sem=send.at[d - 1],
                    recv_sem=recv.at[d - 1],
                    device_id={axis: lax.rem(index + d, size)},
                    device_id_type=MESH,
                )
            )
            copies[-1].start()
        return copies

    def collect(size, index, src, buf, copies):
        buf[index] = src[...]
        for copy in copies:
            copy.wait()
        total = buf[0]
        for n in range(1, size):
            total = total + buf[n]
        return total

    pcopies = exchange("row", count, row, proj_ref, prow_ref, psend, precv)

    psum_ref[...] = collect(count, row, proj_ref, prow_ref, pcopies)
    pncopies = exchange("node", parts, me, psum_ref, pnode_ref, pnsend, pnrecv)
    proj = collect(parts, me, psum_ref, pnode_ref, pncopies)

    lane = lax.broadcasted_iota(jnp.int32, (1, nf), 1) // (2 * cols)
    scale = jnp.zeros((1, nf), jnp.float32)
    for k in range(quad):
        scale = jnp.where(lane == k, weights_ref[k] / quad, scale)
    hi, lo = split(proj * scale)
    pw = jnp.concatenate(
        [jnp.concatenate([hi, hi], 1), jnp.concatenate([lo, jnp.zeros_like(lo)], 1)], 0
    )

    size = min(CHUNK, own)
    per = own // size
    chunks = planes * per

    def respond(ch):
        plane, y0 = ch // per, (ch % per) * size

        def pair(j, c):
            r = plane * own + y0 + 2 * j
            right = jnp.concatenate([f_ref[r], f_ref[r + 1]], 1)
            both = jnp.dot(pw, right, preferred_element_type=jnp.float32)
            both = both[:probes] + both[probes:]
            at = plane * gy + me * own + y0 + 2 * j
            out_ref[pl.ds(at, probes, stride=planes * gy), :] = both[:, :gz]
            out_ref[pl.ds(at + 1, probes, stride=planes * gy), :] = both[:, gz:]
            return c

        lax.fori_loop(0, size // 2, pair, 0)

    def send(ch, owner, target, slot):
        plane, y0 = ch // per, (ch % per) * size
        view = out.at[:, plane, pl.ds(pl.multiple_of(owner * own + y0, 8), size), :]
        return pltpu.make_async_remote_copy(
            src_ref=view,
            dst_ref=view,
            send_sem=osend.at[slot, ch],
            recv_sem=orecv.at[slot, ch],
            device_id={"node": target},
            device_id_type=MESH,
        )

    def spread():
        def products(j, c):
            total = None
            for m in range(MERGE):
                right = pairs(MERGE * j + m)
                part = nt(right[:nf], right)
                total = part if total is None else total + part
            acc_ref[...] += total
            return c

        lax.fori_loop(0, steps, products, 0)
        cross = acc_ref[:, nf:]
        gram = acc_ref[:, :nf] + cross + cross.T
        block = lax.broadcasted_iota(jnp.int32, (cols, nf), 1) // cols
        diag = jnp.zeros((cols, nf), jnp.float32)
        for n in range(nf // cols):
            diag = diag + jnp.where(block == n, gram[n * cols : (n + 1) * cols], 0.0)
        part_ref[...] = diag
        gcopies = exchange("row", count, row, part_ref, grow_ref, gsend, grecv)
        gsum_ref[...] = collect(count, row, part_ref, grow_ref, gcopies)
        return exchange("node", parts, me, gsum_ref, gnode_ref, gnsend, gnrecv)

    started = []
    if parts == 4:
        near = me + 1 - 2 * lax.rem(me, 2)
        far = lax.rem(me + 2, 4)

        def launch(ch):
            for slot, target in ((0, near), (1, far)):
                copy = send(ch, me, target, slot)
                copy.start()
                started.append(copy)

        respond(0)
        for ch in range(1, chunks):
            respond(ch)
            launch(ch - 1)
        launch(chunks - 1)
        gncopies = spread()
        for ch in range(chunks):
            a, b = send(ch, near, near, 0), send(ch, far, far, 1)
            a.wait_recv()
            b.wait_recv()
            copy = send(ch, near, far, 2) if ch % 2 else send(ch, far, near, 2)
            copy.start()
            started.append(copy)
    else:
        for ch in range(chunks):
            respond(ch)
            for d in range(1, parts):
                copy = send(ch, me, lax.rem(me + d, parts), d - 1)
                copy.start()
                started.append(copy)

    if parts != 4:
        gncopies = spread()
    diag = collect(parts, me, gsum_ref, gnode_ref, gncopies)
    source = lax.broadcasted_iota(jnp.int32, (nf, cols), 0)
    column = lax.broadcasted_iota(jnp.int32, (nf, cols), 1)
    total = jnp.zeros((cols, cols), jnp.float32)
    for m in range(NODE_DEV):
        node = assign_ref[me * NODE_DEV + m]
        pick = ((source // (2 * cols) == node) & (source % cols == column)).astype(jnp.bfloat16)
        rest = diag
        picked = jnp.zeros((cols, cols), jnp.float32)
        for _ in range(3):
            piece = rest.astype(jnp.bfloat16)
            rest = rest - piece.astype(jnp.float32)
            picked = picked + jnp.dot(piece, pick, preferred_element_type=jnp.float32)
        total = total + weights_ref[node] * picked
    gram_ref[...] = total / cells

    if parts == 4:
        for ch in range(chunks):
            diagonal = lax.rem(near + 2, 4)
            send(ch, diagonal, near, 2).wait_recv()
        for copy in started:
            copy.wait_send()
    else:
        for ch in range(chunks):
            for d in range(1, parts):
                send(ch, lax.rem(me + parts - d, parts), me, d - 1).wait_recv()
        for copy in started:
            copy.wait_send()


def split(v):
    hi = v.astype(jnp.bfloat16)
    return hi, (v - hi.astype(jnp.float32)).astype(jnp.bfloat16)


def local(inputs, diagonal, observations, frequencies, weights, counts, assignment):
    parts = lax.axis_size("node")
    count = lax.axis_size("row")
    cols, planes, gy, gz = inputs.shape
    probes = observations.shape[0]
    quad = frequencies.shape[0]
    own = gy // parts
    halo = ITERS - 1
    win = own + 2 * halo
    size = own + 2 * EDGE
    nf = quad * 2 * cols
    local_rows = planes * own

    total = planes + 2 * halo
    vmem = pl.BlockSpec(memory_space=pltpu.VMEM)
    smem = pl.BlockSpec(memory_space=pltpu.SMEM)
    hbm = pl.BlockSpec(memory_space=pl.ANY)
    dma = pltpu.SemaphoreType.DMA
    src, diag, obs = pl.pallas_call(
        functools.partial(exchange_kernel, halo, own, parts, count),
        out_shape=(
            jax.ShapeDtypeStruct((total, size + 2 * EDGE, cols, gz), jnp.float32),
            jax.ShapeDtypeStruct((total, size, gz), jnp.float32),
            jax.ShapeDtypeStruct((local_rows, probes, gz), jnp.float32),
        ),
        in_specs=[hbm, hbm, hbm],
        out_specs=(vmem, vmem, vmem),
        scratch_shapes=[
            pltpu.VMEM((planes, cols, size, gz), jnp.float32),
            pltpu.VMEM((planes, probes, own, gz), jnp.float32),
            dma((planes,)),
            dma,
            dma((planes,)),
            dma((total + 2,)),
            dma((total,)),
            dma((4,)),
            dma((4,)),
        ],
        compiler_params=pltpu.CompilerParams(
            vmem_limit_bytes=EXCHANGE_VMEM, collective_id=1, has_side_effects=True
        ),
        name="exchange",
    )(*[pltpu.with_memory_space_constraint(x, pltpu.HBM) for x in (inputs, diagonal, observations)])

    fhl = pl.pallas_call(
        functools.partial(sweep_kernel, halo, own, planes),
        out_shape=jax.ShapeDtypeStruct((local_rows, 2, quad, 2, cols, gz), jnp.bfloat16),
        in_specs=[smem, smem, vmem, vmem],
        out_specs=vmem,
        scratch_shapes=[
            pltpu.VMEM((2, total, win + 6, cols, gz), jnp.float32),
            pltpu.VMEM((2, total, win + 6, cols, gz), jnp.float32),
            pltpu.VMEM((2 * gz, gz), jnp.bfloat16),
            pltpu.VMEM((GROUPS, 2, 2, STEP + 2, cols, gz), jnp.float32),
            pltpu.VMEM((total, size + 2 * EDGE, gz), jnp.float32),
            pltpu.VMEM((total, size + 2 * EDGE, gz), jnp.float32),
        ],
        compiler_params=pltpu.CompilerParams(vmem_limit_bytes=SWEEP_VMEM),
        name="sweeps",
    )(counts, frequencies, src, diag)

    cells = planes * gy * gz * count
    chunks = planes * (own // min(CHUNK, own))
    response, group_gram = pl.pallas_call(
        functools.partial(tail_kernel, parts, count, planes, own, cells),
        out_shape=(
            jax.ShapeDtypeStruct((probes * planes * gy, gz), jnp.float32),
            jax.ShapeDtypeStruct((cols, cols), jnp.float32),
        ),
        in_specs=[smem, smem, vmem, vmem],
        out_specs=(vmem, vmem),
        scratch_shapes=[
            pltpu.VMEM((nf, 2 * nf), jnp.float32),
            pltpu.VMEM((2 * nf, 2 * probes), jnp.float32),
            pltpu.VMEM((probes, nf), jnp.float32),
            pltpu.VMEM((cols, nf), jnp.float32),
            pltpu.VMEM((count, probes, nf), jnp.float32),
            pltpu.VMEM((probes, nf), jnp.float32),
            pltpu.VMEM((parts, probes, nf), jnp.float32),
            pltpu.VMEM((count, cols, nf), jnp.float32),
            pltpu.VMEM((cols, nf), jnp.float32),
            pltpu.VMEM((parts, cols, nf), jnp.float32),
            dma((count - 1,)),
            dma((count - 1,)),
            dma((parts - 1,)),
            dma((parts - 1,)),
            dma((count - 1,)),
            dma((count - 1,)),
            dma((parts - 1,)),
            dma((parts - 1,)),
            dma((parts - 1, chunks)),
            dma((parts - 1, chunks)),
        ],
        compiler_params=pltpu.CompilerParams(
            vmem_limit_bytes=TAIL_VMEM, collective_id=0, has_side_effects=True
        ),
        name="tail",
    )(weights, assignment, obs, fhl.reshape(local_rows, 2 * nf, gz))
    return response.reshape(probes, planes, gy, gz), group_gram[None]


def solution(mesh):
    placed = (
        P(None, "row", None, None),
        P("row", None, None),
        P(None, "row", None, None),
        P(),
        P(),
        P(),
        P(),
    )
    return jax.shard_map(
        local,
        mesh=mesh,
        in_specs=placed,
        out_specs=(P(None, "row", None, None), P("node", None, None)),
        check_vma=False,
    )
```

```python
import functools

import jax
import jax.numpy as jnp
from jax import lax
from jax.experimental import pallas as pl
from jax.experimental.pallas import tpu as pltpu
from jax.sharding import PartitionSpec as P

NODE_DEV = 1
ITERS = 6
EXCHANGE_VMEM = 8 * 1024 * 1024
SWEEP_VMEM = 30 * 1024 * 1024
TAIL_VMEM = 16 * 1024 * 1024
STEP = 8
OFF = 1
EDGE = 8
GROUPS = 2
MERGE = 2
SPAN = 8
START = 6
CHUNK = 8
MESH = pl.DeviceIdType.MESH


def exchange_kernel(halo, own, parts, count, inputs, diagonal, observations, src_ref, dg_ref, ob_ref,
                    nat_ref, onat_ref, load_sem, dload_sem, oload_sem, send_sem, recv_sem, dsend_sem, drecv_sem):
    me = lax.axis_index("node")
    row = lax.axis_index("row")
    cols, planes, gy, gz = inputs.shape
    probes = observations.shape[0]
    size = nat_ref.shape[2]
    start = pl.multiple_of(jnp.clip(me * own - EDGE, 0, gy - size), 8)
    top = halo + planes
    last = top + halo - 1

    loads = []
    for j in range(planes):
        loads.append(
            pltpu.make_async_copy(inputs.at[:, j, pl.ds(start, size), :], nat_ref.at[j], load_sem.at[j])
        )
        loads[-1].start()
    dload = pltpu.make_async_copy(
        diagonal.at[:, pl.ds(start, size), :], dg_ref.at[pl.ds(halo, planes)], dload_sem
    )
    dload.start()
    oloads = []
    for j in range(planes):
        rows = pl.ds(pl.multiple_of(me * own, 8), own)
        oloads.append(
            pltpu.make_async_copy(observations.at[:, j, rows, :], onat_ref.at[j], oload_sem.at[j])
        )
        oloads[-1].start()

    barrier = pltpu.get_barrier_semaphore()
    for hop in (-2, -1, 1, 2):
        @pl.when((row + hop >= 0) & (row + hop < count))
        def _():
            pl.semaphore_signal(barrier, inc=1, device_id={"row": row + hop}, device_id_type=MESH)

    def plane(source, target, send, to):
        away = halo - target if target < halo else target - top + 1
        rows = pl.ds(2 * EDGE - halo + away, own + 2 * (halo - away))
        return pltpu.make_async_remote_copy(
            src_ref=src_ref.at[source, rows],
            dst_ref=src_ref.at[target, rows],
            send_sem=send_sem.at[send],
            recv_sem=recv_sem.at[target],
            device_id={"row": to},
            device_id_type=MESH,
        )

    def strip(source, target, size, slot, to):
        return pltpu.make_async_remote_copy(
            src_ref=dg_ref.at[pl.ds(source, size)],
            dst_ref=dg_ref.at[pl.ds(target, size)],
            send_sem=dsend_sem.at[slot],
            recv_sem=drecv_sem.at[slot],
            device_id={"row": to},
            device_id_type=MESH,
        )

    even = lax.rem(row, 2) == 0
    far = halo - planes
    up = [plane(halo + j, far + j, far + j, row + 1) for j in range(planes)]
    up_far = plane(top - 1, 0, 0, row + 2)
    up_pass = plane(halo - 1, 0, last + 1, row + 1)
    down = [plane(halo + j, top + j, top + j, row - 1) for j in range(planes)]
    down_far = plane(halo, last, last, row - 2)
    down_pass = plane(top, last, last + 2, row - 1)
    strips = (
        (row + 1 < count, row >= 1, strip(halo, far, planes, 0, row + 1)),
        (row + 2 < count, row >= 2, strip(top - far, 0, far, 1, row + 2)),
        (row >= 1, row + 1 < count, strip(halo, top, planes, 2, row - 1)),
        (row >= 2, row + 2 < count, strip(halo, top + planes, far, 3, row - 2)),
    )
    has_up, has_down = row + 1 < count, row >= 1
    direct_up, direct_down = even & (row + 2 < count), ~even & (row >= 2)
    pass_up, pass_down = even & has_down & has_up, ~even & has_up & has_down

    def when(flag, *actions):
        @pl.when(flag)
        def _():
            for action in actions:
                action()

    base = start - (me * own - 2 * EDGE)

    def turn(j):
        loads[j].wait()

        def block(o, c):
            at = pl.multiple_of(8 * o, 8)
            for h in range(cols // 8):
                value = nat_ref[j, 8 * h : 8 * h + 8, pl.ds(at, 8), :]
                src_ref[halo + j, pl.ds(base + at, 8), 8 * h : 8 * h + 8, :] = jnp.swapaxes(value, 0, 1)
            return c

        lax.fori_loop(0, size // 8, block, 0)

    def blank(p, at, n):
        src_ref[p, at : at + n] = jnp.zeros((n,) + src_ref.shape[2:], jnp.float32)

    for j in range(planes):
        when(me == 0, lambda: blank(halo + j, EDGE, EDGE))
        when(me == parts - 1, lambda: blank(halo + j, own + 2 * EDGE, EDGE))
    dload.wait()
    pl.semaphore_wait(barrier, jnp.minimum(row, 2) + jnp.minimum(count - 1 - row, 2))
    for sends, _, copy in strips:
        when(sends, copy.start)
    turn(planes - 1)
    turn(0)
    for n in range(1, planes):
        if n + 1 < planes:
            turn(planes - 1 - n)
        when(has_up, up[planes - n].start)
        when(has_down, down[n - 1].start)
        if n == 1:
            when(direct_up, up_far.start)
            when(direct_down, down_far.start)
    when(has_up, up[0].start)
    when(has_down, down[planes - 1].start)

    for away in range(1, halo + 1):
        for p in (halo - away, top - 1 + away):
            blank(p, 2 * EDGE - halo, away)
            blank(p, own + 2 * EDGE + halo - away, away)

    for copy in oloads:
        copy.wait()

    def probe(n, c):
        p, at = n // (own // 8), pl.multiple_of(lax.rem(n, own // 8) * 8, 8)
        for h in range(probes // 8):
            value = jnp.swapaxes(onat_ref[p, 8 * h : 8 * h + 8, pl.ds(at, 8), :], 0, 1)
            ob_ref[pl.ds(8 * n, 8), 8 * h : 8 * h + 8, :] = value
        return c

    lax.fori_loop(0, planes * (own // 8), probe, 0)

    when(has_down, up[-1].wait_recv)
    when(pass_up, up_pass.start)
    when(has_up, down[0].wait_recv)
    when(pass_down, down_pass.start)
    for j in range(1, planes):
        when(has_down, up[planes - 1 - j].wait_recv)
        when(has_up, down[j].wait_recv)
    when(row >= 2, up_far.wait_recv)
    when(row + 2 < count, down_far.wait_recv)
    for _, receives, copy in strips:
        when(receives, copy.wait_recv)

    def clear(at, n):
        def one(p, c):
            src_ref[p] = jnp.zeros(src_ref.shape[1:], jnp.float32)
            dg_ref[p] = jnp.zeros(dg_ref.shape[1:], jnp.float32)
            return c

        return lambda: lax.fori_loop(at, at + n, one, 0)

    when(row < 1, clear(far, planes))
    when(row < 2, clear(0, far))
    when(row + 1 >= count, clear(top, planes))
    when(row + 2 >= count, clear(top + planes, far))

    when(has_up, *[copy.wait_send for copy in up])
    when(has_down, *[copy.wait_send for copy in down])
    when(direct_up, up_far.wait_send)
    when(direct_down, down_far.wait_send)
    when(pass_up, up_pass.wait_send)
    when(pass_down, down_pass.wait_send)
    for sends, _, copy in strips:
        when(sends, copy.wait_send)


def sweep_kernel(halo, own, planes, counts_ref, freq_ref, src_ref, dg_ref, fhl_ref,
                 xa_ref, xb_ref, near_ref, st_ref, gr_ref, gi_ref):
    total = planes + 2 * halo
    cols, gz = src_ref.shape[2:]
    quad = counts_ref.shape[0]
    size = dg_ref.shape[1]
    me = lax.axis_index("node")
    start = jnp.clip(me * own - EDGE, 0, own * lax.axis_size("node") - size)
    lift = me * own - halo - OFF - start + EDGE
    skew = 2 * EDGE - halo - OFF

    gap = lax.broadcasted_iota(jnp.int32, (2 * gz, gz), 0) % gz - lax.broadcasted_iota(
        jnp.int32, (2 * gz, gz), 1
    )
    near_ref[...] = ((gap == 1) | (gap == -1)).astype(jnp.bfloat16)
    lane = lax.broadcasted_iota(jnp.int32, (cols, gz), 1)
    first = lane == 0
    last = lane == gz - 1

    def beside(v):
        return jnp.where(first, 0.0, pltpu.roll(v, 1, 1)) + jnp.where(
            last, 0.0, pltpu.roll(v, gz - 1, 1)
        )

    def gain(p, y):
        return (
            jnp.broadcast_to(gr_ref[p, pl.ds(y + lift, 1), :], (cols, gz)),
            jnp.broadcast_to(gi_ref[p, pl.ds(y + lift, 1), :], (cols, gz)),
        )

    def stage(x_ref, spots, parity):
        for g, (p, y) in enumerate(spots):
            us = [[x_ref[0, p + q, y - 1 + t] for t in range(STEP + 2)] for q in range(2)]
            for t in range(STEP):
                for q in range(2):
                    n = (us[q][t] + us[q][t + 2]) + (us[1 - q][t + 1] + src_ref[p + q, y + skew + t])
                    st_ref[g, 0, q, parity + t] = n + beside(us[q][t + 1])
        left, sums = [], []
        for g, (p, y) in enumerate(spots):
            ws = [[x_ref[1, p + q, y - 1 + t] for t in range(STEP + 2)] for q in range(2)]
            for t in range(STEP):
                for q in range(2):
                    hi, lo = split(ws[q][t + 1])
                    left.append(jnp.concatenate([hi, lo], 1))
        z = jnp.dot(jnp.concatenate(left, 0), near_ref[...], preferred_element_type=jnp.float32)
        for g, (p, y) in enumerate(spots):
            ws = [[x_ref[1, p + q, y - 1 + t] for t in range(STEP + 2)] for q in range(2)]
            for t in range(STEP):
                for q in range(2):
                    n = (ws[q][t] + ws[q][t + 2]) + ws[1 - q][t + 1]
                    at = (2 * (STEP * g + t) + q) * cols
                    st_ref[g, 1, q, parity + t] = n + z[at : at + cols]

    def combine(x_ref, spots, put, parity):
        for g, (p, y) in enumerate(spots):
            for t in range(STEP):
                for q in range(2):
                    side = p + 3 * q - 1
                    nu = st_ref[g, 0, q, parity + t] + x_ref[0, side, y + t]
                    nw = st_ref[g, 1, q, parity + t] + x_ref[1, side, y + t]
                    gr, gi = gain(p + q, y + t)
                    put(p + q, y + t, gr * nu - gi * nw, gr * nw + gi * nu)

    def sweep(x_ref, radius, put):
        first_plane = halo - radius
        low = first_plane + OFF
        parity = lax.rem(low, 2)
        groups = (own + 2 * radius + STEP - 1) // STEP
        end = low + STEP * groups
        top = first_plane + planes + 2 * radius - 2
        pairs = (planes + 2 * radius) // 2

        def after(p, y):
            wrap = y + STEP >= end
            past = p + 2 > top
            ny = jnp.where(wrap, jnp.where(past, y, low), y + STEP)
            return jnp.where(wrap & ~past, p + 2, p), ny

        spots = [(first_plane, low)]
        for _ in range(GROUPS - 1):
            spots.append(after(*spots[-1]))
        stage(x_ref, spots, parity)

        def body(j, spots):
            nxt = [after(*spots[-1])]
            for _ in range(GROUPS - 1):
                nxt.append(after(*nxt[-1]))
            combine(x_ref, spots, put, parity)
            stage(x_ref, nxt, parity)
            return tuple(nxt)

        lax.fori_loop(0, (groups * pairs + GROUPS - 1) // GROUPS, body, tuple(spots))

    def node(k, c):
        w = freq_ref[k]
        count = counts_ref[k]
        low1 = halo + 1 - count

        def gains(p, c):
            part = dg_ref[p]
            d = 6.0 + part
            inv = jnp.where(part > 0.0, 1.0 / (d * d + w * w), 0.0)
            rows = slice(EDGE, EDGE + size)
            for ref, value in ((gr_ref, d * inv), (gi_ref, -w * inv)):
                ref[p, :EDGE] = jnp.zeros((EDGE, gz), jnp.float32)
                ref[p, rows] = value
                ref[p, EDGE + size :] = jnp.zeros((EDGE, gz), jnp.float32)
            return c

        lax.fori_loop(low1, total - low1, gains, 0)

        groups1 = (own + 2 * (count - 1) + START - 1) // START

        def start_planes(n, c):
            def rows(j, c):
                y = low1 + OFF + START * j
                for t in range(START):
                    for q in range(2):
                        p = low1 + 2 * n + q
                        b = src_ref[p, y + skew + t]
                        gr, gi = gain(p, y + t)
                        xa_ref[0, p, y + t] = gr * b
                        xa_ref[1, p, y + t] = gi * b
                return c

            return lax.fori_loop(0, groups1, rows, c)

        lax.fori_loop(0, planes // 2 + count - 1, start_planes, 0)

        def into(ref):
            def put(p, y, u, v):
                ref[0, p, y] = u
                ref[1, p, y] = v

            return put

        def put_last(p, y, u, v):
            row = (p - halo) * own + (y - halo - OFF)
            for comp, value in ((0, u), (1, v)):
                hi, lo = split(value)
                fhl_ref[row, 0, k, comp] = hi
                fhl_ref[row, 1, k, comp] = lo

        inner = count - 2

        def pair(i, c):
            s = 2 * i + 2
            sweep(xa_ref, count - s, into(xb_ref))

            @pl.when(2 * i + 1 < inner)
            def _():
                sweep(xb_ref, count - s - 1, into(xa_ref))

            return c

        lax.fori_loop(0, (inner + 1) // 2, pair, 0)

        @pl.when(inner % 2 == 1)
        def _():
            sweep(xb_ref, 0, put_last)

        @pl.when(inner % 2 == 0)
        def _():
            sweep(xa_ref, 0, put_last)

        return c

    lax.fori_loop(0, quad, node, 0)


def tail_kernel(parts, count, planes, own, cells, weights_ref, assign_ref, obs_ref, f_ref,
                out_ref, gram_ref, acc_ref, pt_ref, proj_ref, part_ref, prow_ref, psum_ref, pnode_ref, grow_ref, gsum_ref, gnode_ref,
                psend, precv, pnsend, pnrecv, gsend, grecv, gnsend, gnrecv, osend, orecv):
    me = lax.axis_index("node")
    row = lax.axis_index("row")
    probes, nf = proj_ref.shape
    cols = part_ref.shape[0]
    quad = weights_ref.shape[0]
    gz = out_ref.shape[1]
    gy = own * parts
    out = out_ref.reshape(probes, planes, gy, gz)

    barrier = pltpu.get_barrier_semaphore()
    for d in range(1, count):
        pl.semaphore_signal(barrier, inc=1, device_id={"row": lax.rem(row + d, count)}, device_id_type=MESH)
    for d in range(1, parts):
        pl.semaphore_signal(barrier, inc=1, device_id={"node": lax.rem(me + d, parts)}, device_id_type=MESH)

    def pairs(j):
        r = 2 * j
        return jnp.concatenate([f_ref[r], f_ref[r + 1]], 1)

    def nt(left, right):
        return lax.dot_general(left, right, (((1,), (1,)), ((), ())), preferred_element_type=jnp.float32)

    def probe(n):
        his, los = zip(split(obs_ref[2 * n]), split(obs_ref[2 * n + 1]))
        return jnp.concatenate([jnp.concatenate(his, 1), jnp.concatenate(los, 1)], 0)

    def project(j, c):
        n = SPAN * j
        left = jnp.concatenate([pairs(n + m) for m in range(SPAN)], 1)
        pt_ref[...] += nt(left, jnp.concatenate([probe(n + m) for m in range(SPAN)], 1))
        return c

    steps = f_ref.shape[0] // (2 * MERGE)
    pt_ref[...] = jnp.zeros_like(pt_ref)
    lax.fori_loop(0, f_ref.shape[0] // (2 * SPAN), project, 0)
    both = pt_ref[...].T
    proj_ref[...] = both[:probes, :nf] + both[probes:, :nf] + both[:probes, nf:]
    acc_ref[...] = jnp.zeros_like(acc_ref)
    pl.semaphore_wait(barrier, count - 1 + parts - 1)

    def exchange(axis, size, index, src, buf, send, recv):
        copies = []
        for d in range(1, size):
            copies.append(
                pltpu.make_async_remote_copy(
                    src_ref=src,
                    dst_ref=buf.at[index],
                    send_sem=send.at[d - 1],
                    recv_sem=recv.at[d - 1],
                    device_id={axis: lax.rem(index + d, size)},
                    device_id_type=MESH,
                )
            )
            copies[-1].start()
        return copies

    def collect(size, index, src, buf, copies):
        buf[index] = src[...]
        for copy in copies:
            copy.wait()
        total = buf[0]
        for n in range(1, size):
            total = total + buf[n]
        return total

    pcopies = exchange("row", count, row, proj_ref, prow_ref, psend, precv)

    psum_ref[...] = collect(count, row, proj_ref, prow_ref, pcopies)
    pncopies = exchange("node", parts, me, psum_ref, pnode_ref, pnsend, pnrecv)
    proj = collect(parts, me, psum_ref, pnode_ref, pncopies)

    lane = lax.broadcasted_iota(jnp.int32, (1, nf), 1) // (2 * cols)
    scale = jnp.zeros((1, nf), jnp.float32)
    for k in range(quad):
        scale = jnp.where(lane == k, weights_ref[k] / quad, scale)
    hi, lo = split(proj * scale)
    pw = jnp.concatenate(
        [jnp.concatenate([hi, hi], 1), jnp.concatenate([lo, jnp.zeros_like(lo)], 1)], 0
    )

    size = min(CHUNK, own)
    per = own // size
    chunks = planes * per

    def respond(ch):
        plane, y0 = ch // per, (ch % per) * size

        def pair(j, c):
            r = plane * own + y0 + 2 * j
            right = jnp.concatenate([f_ref[r], f_ref[r + 1]], 1)
            both = jnp.dot(pw, right, preferred_element_type=jnp.float32)
            both = both[:probes] + both[probes:]
            at = plane * gy + me * own + y0 + 2 * j
            out_ref[pl.ds(at, probes, stride=planes * gy), :] = both[:, :gz]
            out_ref[pl.ds(at + 1, probes, stride=planes * gy), :] = both[:, gz:]
            return c

        lax.fori_loop(0, size // 2, pair, 0)

    def send(ch, owner, target, slot):
        plane, y0 = ch // per, (ch % per) * size
        view = out.at[:, plane, pl.ds(pl.multiple_of(owner * own + y0, 8), size), :]
        return pltpu.make_async_remote_copy(
            src_ref=view,
            dst_ref=view,
            send_sem=osend.at[slot, ch],
            recv_sem=orecv.at[slot, ch],
            device_id={"node": target},
            device_id_type=MESH,
        )

    def spread():
        def products(j, c):
            total = None
            for m in range(MERGE):
                right = pairs(MERGE * j + m)
                part = nt(right[:nf], right)
                total = part if total is None else total + part
            acc_ref[...] += total
            return c

        lax.fori_loop(0, steps, products, 0)
        cross = acc_ref[:, nf:]
        gram = acc_ref[:, :nf] + cross + cross.T
        block = lax.broadcasted_iota(jnp.int32, (cols, nf), 1) // cols
        diag = jnp.zeros((cols, nf), jnp.float32)
        for n in range(nf // cols):
            diag = diag + jnp.where(block == n, gram[n * cols : (n + 1) * cols], 0.0)
        part_ref[...] = diag
        gcopies = exchange("row", count, row, part_ref, grow_ref, gsend, grecv)
        gsum_ref[...] = collect(count, row, part_ref, grow_ref, gcopies)
        return exchange("node", parts, me, gsum_ref, gnode_ref, gnsend, gnrecv)

    started = []
    if parts == 4:
        near = me + 1 - 2 * lax.rem(me, 2)
        far = lax.rem(me + 2, 4)

        def launch(ch):
            for slot, target in ((0, near), (1, far)):
                copy = send(ch, me, target, slot)
                copy.start()
                started.append(copy)

        respond(0)
        for ch in range(1, chunks):
            respond(ch)
            launch(ch - 1)
        launch(chunks - 1)
        gncopies = spread()
        for ch in range(chunks):
            a, b = send(ch, near, near, 0), send(ch, far, far, 1)
            a.wait_recv()
            b.wait_recv()
            copy = send(ch, near, far, 2) if ch % 2 else send(ch, far, near, 2)
            copy.start()
            started.append(copy)
    else:
        for ch in range(chunks):
            respond(ch)
            for d in range(1, parts):
                copy = send(ch, me, lax.rem(me + d, parts), d - 1)
                copy.start()
                started.append(copy)

    if parts != 4:
        gncopies = spread()
    diag = collect(parts, me, gsum_ref, gnode_ref, gncopies)
    source = lax.broadcasted_iota(jnp.int32, (nf, cols), 0)
    column = lax.broadcasted_iota(jnp.int32, (nf, cols), 1)
    total = jnp.zeros((cols, cols), jnp.float32)
    for m in range(NODE_DEV):
        node = assign_ref[me * NODE_DEV + m]
        pick = ((source // (2 * cols) == node) & (source % cols == column)).astype(jnp.bfloat16)
        rest = diag
        picked = jnp.zeros((cols, cols), jnp.float32)
        for _ in range(3):
            piece = rest.astype(jnp.bfloat16)
            rest = rest - piece.astype(jnp.float32)
            picked = picked + jnp.dot(piece, pick, preferred_element_type=jnp.float32)
        total = total + weights_ref[node] * picked
    gram_ref[...] = total / cells

    if parts == 4:
        for ch in range(chunks):
            diagonal = lax.rem(near + 2, 4)
            send(ch, diagonal, near, 2).wait_recv()
        for copy in started:
            copy.wait_send()
    else:
        for ch in range(chunks):
            for d in range(1, parts):
                send(ch, lax.rem(me + parts - d, parts), me, d - 1).wait_recv()
        for copy in started:
            copy.wait_send()


def split(v):
    hi = v.astype(jnp.bfloat16)
    return hi, (v - hi.astype(jnp.float32)).astype(jnp.bfloat16)


def local(inputs, diagonal, observations, frequencies, weights, counts, assignment):
    parts = lax.axis_size("node")
    count = lax.axis_size("row")
    cols, planes, gy, gz = inputs.shape
    probes = observations.shape[0]
    quad = frequencies.shape[0]
    own = gy // parts
    halo = ITERS - 1
    win = own + 2 * halo
    size = own + 2 * EDGE
    nf = quad * 2 * cols
    local_rows = planes * own

    total = planes + 2 * halo
    vmem = pl.BlockSpec(memory_space=pltpu.VMEM)
    smem = pl.BlockSpec(memory_space=pltpu.SMEM)
    hbm = pl.BlockSpec(memory_space=pl.ANY)
    dma = pltpu.SemaphoreType.DMA
    src, diag, obs = pl.pallas_call(
        functools.partial(exchange_kernel, halo, own, parts, count),
        out_shape=(
            jax.ShapeDtypeStruct((total, size + 2 * EDGE, cols, gz), jnp.float32),
            jax.ShapeDtypeStruct((total, size, gz), jnp.float32),
            jax.ShapeDtypeStruct((local_rows, probes, gz), jnp.float32),
        ),
        in_specs=[hbm, hbm, hbm],
        out_specs=(vmem, vmem, vmem),
        scratch_shapes=[
            pltpu.VMEM((planes, cols, size, gz), jnp.float32),
            pltpu.VMEM((planes, probes, own, gz), jnp.float32),
            dma((planes,)),
            dma,
            dma((planes,)),
            dma((total + 2,)),
            dma((total,)),
            dma((4,)),
            dma((4,)),
        ],
        compiler_params=pltpu.CompilerParams(
            vmem_limit_bytes=EXCHANGE_VMEM, collective_id=1, has_side_effects=True
        ),
        name="exchange",
    )(*[pltpu.with_memory_space_constraint(x, pltpu.HBM) for x in (inputs, diagonal, observations)])

    fhl = pl.pallas_call(
        functools.partial(sweep_kernel, halo, own, planes),
        out_shape=jax.ShapeDtypeStruct((local_rows, 2, quad, 2, cols, gz), jnp.bfloat16),
        in_specs=[smem, smem, vmem, vmem],
        out_specs=vmem,
        scratch_shapes=[
            pltpu.VMEM((2, total, win + 6, cols, gz), jnp.float32),
            pltpu.VMEM((2, total, win + 6, cols, gz), jnp.float32),
            pltpu.VMEM((2 * gz, gz), jnp.bfloat16),
            pltpu.VMEM((GROUPS, 2, 2, STEP + 2, cols, gz), jnp.float32),
            pltpu.VMEM((total, size + 2 * EDGE, gz), jnp.float32),
            pltpu.VMEM((total, size + 2 * EDGE, gz), jnp.float32),
        ],
        compiler_params=pltpu.CompilerParams(vmem_limit_bytes=SWEEP_VMEM),
        name="sweeps",
    )(counts, frequencies, src, diag)

    cells = planes * gy * gz * count
    chunks = planes * (own // min(CHUNK, own))
    response, group_gram = pl.pallas_call(
        functools.partial(tail_kernel, parts, count, planes, own, cells),
        out_shape=(
            jax.ShapeDtypeStruct((probes * planes * gy, gz), jnp.float32),
            jax.ShapeDtypeStruct((cols, cols), jnp.float32),
        ),
        in_specs=[smem, smem, vmem, vmem],
        out_specs=(vmem, vmem),
        scratch_shapes=[
            pltpu.VMEM((nf, 2 * nf), jnp.float32),
            pltpu.VMEM((2 * nf, 2 * probes), jnp.float32),
            pltpu.VMEM((probes, nf), jnp.float32),
            pltpu.VMEM((cols, nf), jnp.float32),
            pltpu.VMEM((count, probes, nf), jnp.float32),
            pltpu.VMEM((probes, nf), jnp.float32),
            pltpu.VMEM((parts, probes, nf), jnp.float32),
            pltpu.VMEM((count, cols, nf), jnp.float32),
            pltpu.VMEM((cols, nf), jnp.float32),
            pltpu.VMEM((parts, cols, nf), jnp.float32),
            dma((count - 1,)),
            dma((count - 1,)),
            dma((parts - 1,)),
            dma((parts - 1,)),
            dma((count - 1,)),
            dma((count - 1,)),
            dma((parts - 1,)),
            dma((parts - 1,)),
            dma((parts - 1, chunks)),
            dma((parts - 1, chunks)),
        ],
        compiler_params=pltpu.CompilerParams(
            vmem_limit_bytes=TAIL_VMEM, collective_id=0, has_side_effects=True
        ),
        name="tail",
    )(weights, assignment, obs, fhl.reshape(local_rows, 2 * nf, gz))
    return response.reshape(probes, planes, gy, gz), group_gram[None]


def solution(mesh):
    placed = (
        P(None, "row", None, None),
        P("row", None, None),
        P(None, "row", None, None),
        P(),
        P(),
        P(),
        P(),
    )
    return jax.shard_map(
        local,
        mesh=mesh,
        in_specs=placed,
        out_specs=(P(None, "row", None, None), P("node", None, None)),
        check_vma=False,
    )
```
